32 devices in a mesh: row: 4 (over y, core), col: 4 (over z), dp: 2 (over x).
Axes of the slice: x: 2, y: 2, z: 4, core: 2. Of those that a mesh axis runs over, the one named last changes fastest.
Arguments:
- slides: bfloat16 [2, 64, 128, 512], P('dp', 'row', 'col'), may hold values from -6 to 6
- cotangent: bfloat16 [2, 64, 128, 512], P('dp', 'row', 'col'), may hold values from -6 to 6
- kernel: float32 [2, 7, 7, 512], replicated, may hold values from -0.875 to 0.875
- kernel_bias: float32 [2, 512], replicated, may hold values from -3 to 3
- norm_gain: float32 [2, 512], replicated, may hold values from 0.1 to 1.9
- norm_bias: float32 [2, 512], replicated, may hold values from -3 to 3
- weight_in: bfloat16 [2, 512, 2048], P(None, 'dp'), may hold values from -0.25 to 0.25
- bias_in: float32 [2, 2048], replicated, may hold values from -3 to 3
- weight_out: bfloat16 [2, 2048, 512], P(None, None, 'dp'), may hold values from -0.125 to 0.125
- bias_out: float32 [2, 512], replicated, may hold values from -3 to 3
- layer_scale: float32 [2, 512], replicated, may hold values from 0.3 to 1.5
Outputs:
- output: bfloat16 [2, 64, 128, 512], P('dp', 'row', 'col')
- grad_slides: bfloat16 [2, 64, 128, 512], P('dp', 'row', 'col')
- grad_weight_in: float32 [2, 512, 2048], P(None, 'dp')
- grad_weight_out: float32 [2, 2048, 512], P(None, None, 'dp')
- grad_kernel: float32 [2, 7, 7, 512], replicated
- grad_channel: float32 [2, 5, 512], replicated
- grad_bias_in: float32 [2, 2048], replicated
The draws below stay inside these ranges and needn't reach their ends.
All inputs are finite; a program needn't handle non-finite values.
Results may differ from the reference program's by a relative error of at most 0.01.
Values may be sent and summed in bfloat16 or wider, within the bound.
A program may use at most 128 MiB of HBM per device.

```python
import math
import jax
import jax.numpy as jnp
from jax import lax

D = 512
FF = 2048
LAYERS = 2
SLIDES = 2
HEIGHT = 64
WIDTH = 128


def shard_levels(rng, shape, pieces, smallest, high):
    def one(position, blocks):
        steps = jax.random.uniform(jax.random.fold_in(jax.random.fold_in(rng, 6), position), (blocks,), jnp.float32, smallest / len(pieces), high / len(pieces))
        return jnp.repeat(jnp.exp(steps), shape[position] // blocks).reshape((-1,) + (1,) * (len(shape) - position - 1))

    loudness = one(*pieces[0])
    for cut in pieces[1:]:
        loudness = loudness * one(*cut)
    return loudness


def normal_values(key, dims, spread, reach, cuts=(), held_as=jnp.bfloat16):
    factor_of = shard_levels(key, dims, cuts, -0.22, 0.18) if cuts else 1.0
    entries = jax.random.normal(key, dims, jnp.float32) * spread * factor_of
    return jnp.minimum(jnp.maximum(entries, -reach), reach).astype(held_as)


def setup_inputs(seed: int = 0) -> dict:
    key_list = jax.random.split(jax.random.key(seed), 12)
    slides = normal_values(key_list[0], (SLIDES, HEIGHT, WIDTH, D), 1.0, 6.0, ((0, 2), (1, 4), (2, 4)))
    cotangent = normal_values(key_list[1], (SLIDES, HEIGHT, WIDTH, D), 1.0, 6.0, ((0, 2), (1, 4), (2, 4)))
    kernel = normal_values(key_list[2], (LAYERS, 7, 7, D), 49 ** -0.5, 0.875, (), jnp.float32)
    kernel_bias = normal_values(key_list[3], (LAYERS, D), 0.5, 3.0, (), jnp.float32)
    norm_gain = jnp.clip(1.0 + 0.18 * jax.random.normal(key_list[4], (LAYERS, D), jnp.float32), 0.1, 1.9)
    norm_bias = normal_values(key_list[5], (LAYERS, D), 0.5, 3.0, (), jnp.float32)
    weight_in = normal_values(key_list[6], (LAYERS, D, FF), D ** -0.5, 0.25, ((1, 2),))
    bias_in = normal_values(key_list[7], (LAYERS, FF), 0.5, 3.0, (), jnp.float32)
    weight_out = normal_values(key_list[8], (LAYERS, FF, D), FF ** -0.5, 0.125, ((2, 2),))
    bias_out = normal_values(key_list[9], (LAYERS, D), 0.5, 3.0, (), jnp.float32)
    layer_scale = jnp.clip(jnp.exp(jax.random.uniform(key_list[10], (LAYERS, D), jnp.float32, math.log(0.3), math.log(1.5))), 0.3, 1.5)
    return dict(slides=slides, cotangent=cotangent, kernel=kernel, kernel_bias=kernel_bias, norm_gain=norm_gain, norm_bias=norm_bias, weight_in=weight_in, bias_in=bias_in, weight_out=weight_out, bias_out=bias_out, layer_scale=layer_scale)


COEF = 0.7978845608028654
CUBIC = 0.044715
EPSILON = 1e-06

def gelu_tanh(values):
    inner = COEF * (values + CUBIC * values * values * values)
    return 0.5 * values * (1.0 + jnp.tanh(inner))

def gelu_slope(values):
    tangent = jnp.tanh(COEF * (values + CUBIC * values * values * values))
    return 0.5 * (1.0 + tangent) + 0.5 * values * (1.0 - tangent * tangent) * COEF * (1.0 + 3.0 * CUBIC * values * values)

def depthwise(padded, taps):
    height = padded.shape[1] - 6
    width = padded.shape[2] - 6
    total = jnp.zeros((padded.shape[0], height, width, padded.shape[3]), jnp.float32)
    for row_tap in range(7):
        for col_tap in range(7):
            window = padded[:, row_tap:row_tap + height, col_tap:col_tap + width, :].astype(jnp.float32)
            total = total + window * taps[row_tap, col_tap]
    return total

def tap_grads(padded, upstream):
    height = upstream.shape[1]
    width = upstream.shape[2]
    rows_out = []
    for row_tap in range(7):
        line = []
        for col_tap in range(7):
            window = padded[:, row_tap:row_tap + height, col_tap:col_tap + width, :].astype(jnp.float32)
            line.append(lax.optimization_barrier(jnp.sum(window * upstream, axis=(0, 1, 2))))
        rows_out.append(jnp.stack(line))
    return jnp.stack(rows_out)

def forward_layer(padded, current, taps, tap_bias, gain, shift, weight_in, bias_in, weight_out, bias_out, scale):
    channels = current.shape[-1]
    mixed = (depthwise(padded, taps) + tap_bias).reshape(-1, channels)
    center = mixed - lax.optimization_barrier(jnp.mean(mixed, -1, keepdims=True))
    rstd = lax.rsqrt(lax.optimization_barrier(jnp.mean(center * center, -1, keepdims=True)) + EPSILON)
    normed = center * rstd
    normal_low = (normed * gain + shift).astype(jnp.bfloat16)
    hidden = jnp.dot(normal_low, weight_in, preferred_element_type=jnp.float32) + bias_in
    activated = gelu_tanh(hidden).astype(jnp.bfloat16)
    branch = jnp.dot(activated, weight_out, preferred_element_type=jnp.float32) + bias_out
    result = current.reshape(-1, channels).astype(jnp.float32) + scale * branch
    result = result.astype(jnp.bfloat16).reshape(current.shape)
    return (result, (normed, rstd, normal_low, hidden, activated, branch))

def backward_layer(upstream, saved, gain, weight_in, weight_out, scale):
    normed, rstd, normal_low, hidden, activated, branch = saved
    contract_rows = (((0,), (0,)), ((), ()))
    contract_cols = (((1,), (1,)), ((), ()))
    grad_scale = lax.optimization_barrier(jnp.sum(upstream * branch, 0))
    grad_branch = upstream * scale
    grad_bias_out = lax.optimization_barrier(jnp.sum(grad_branch, 0))
    branch_low = grad_branch.astype(jnp.bfloat16)
    grad_weight_out = lax.dot_general(activated, branch_low, contract_rows, preferred_element_type=jnp.float32)
    grad_act = lax.dot_general(branch_low, weight_out, contract_cols, preferred_element_type=jnp.float32)
    grad_hidden = grad_act * gelu_slope(hidden)
    grad_bias_in = lax.optimization_barrier(jnp.sum(grad_hidden, 0))
    hidden_low = grad_hidden.astype(jnp.bfloat16)
    grad_weight_in = lax.dot_general(normal_low, hidden_low, contract_rows, preferred_element_type=jnp.float32)
    grad_normal = lax.dot_general(hidden_low, weight_in, contract_cols, preferred_element_type=jnp.float32)
    grad_gain = lax.optimization_barrier(jnp.sum(grad_normal * normed, 0))
    grad_shift = lax.optimization_barrier(jnp.sum(grad_normal, 0))
    scaled = grad_normal * gain
    grad_mixed = rstd * (scaled - lax.optimization_barrier(jnp.mean(scaled, -1, keepdims=True)) - normed * lax.optimization_barrier(jnp.mean(scaled * normed, -1, keepdims=True)))
    grad_tap_bias = lax.optimization_barrier(jnp.sum(grad_mixed, 0))
    channel_grads = jnp.stack([grad_tap_bias, grad_gain, grad_shift, grad_bias_out, grad_scale])
    return (grad_mixed, grad_weight_in, grad_weight_out, grad_bias_in, channel_grads)

def pad_map(values):
    return jnp.pad(values, ((0, 0), (3, 3), (3, 3), (0, 0)))

def reference(slides, cotangent, kernel, kernel_bias, norm_gain, norm_bias, weight_in, bias_in, weight_out, bias_out, layer_scale):
    layers = weight_in.shape[0]
    channels = slides.shape[-1]
    current = slides
    caches = []
    paddings = []
    for which in range(layers):
        padded = pad_map(current)
        current, cache = forward_layer(padded, current, kernel[which], kernel_bias[which], norm_gain[which], norm_bias[which], weight_in[which], bias_in[which], weight_out[which], bias_out[which], layer_scale[which])
        caches.append(cache)
        paddings.append(padded)
    output = current
    upstream = cotangent.astype(jnp.float32).reshape(-1, channels)
    grads_in = [None] * layers
    grads_out = [None] * layers
    grads_kernel = [None] * layers
    grads_channel = [None] * layers
    grads_bias = [None] * layers
    for which in reversed(range(layers)):
        grad_mixed, grad_in, grad_out, grad_bias, channel_grads = backward_layer(upstream, caches[which], norm_gain[which], weight_in[which], weight_out[which], layer_scale[which])
        shaped = grad_mixed.reshape(slides.shape)
        grads_kernel[which] = tap_grads(paddings[which], shaped)
        back = depthwise(pad_map(shaped), kernel[which][::-1, ::-1])
        upstream = upstream + back.reshape(-1, channels)
        grads_in[which] = grad_in
        grads_out[which] = grad_out
        grads_channel[which] = channel_grads
        grads_bias[which] = grad_bias
    grad_slides = upstream.astype(jnp.bfloat16).reshape(slides.shape)
    return (output, grad_slides, jnp.stack(grads_in), jnp.stack(grads_out), jnp.stack(grads_kernel), jnp.stack(grads_channel), jnp.stack(grads_bias))
```

```python
import functools

import jax
import jax.numpy as jnp
from jax import lax
from jax.experimental import pallas as pl
from jax.experimental.pallas import tpu as pltpu
from jax.sharding import PartitionSpec as P

COEF = 0.7978845608028654
CUBIC = 0.044715
EPSILON = 1e-06
LANES = 128
UNIT = 16
LEFT = 8
QUARTERS = 4
MESH = pl.DeviceIdType.MESH
F32 = jnp.float32
BF16 = jnp.bfloat16
STRAIGHT = ((-1, 0), (1, 0), (0, -1), (0, 1))
DIAGONAL = ((-1, -1), (-1, 1), (1, -1), (1, 1))
ROWS = (((0,), (0,)), ((), ()))
COLS = (((1,), (1,)), ((), ()))


def step_body(
    sizes,
    slides,
    cotangent,
    kernel,
    kernel_bias,
    norm_gain,
    norm_bias,
    weight_in,
    bias_in,
    weight_out,
    bias_out,
    layer_scale,
    output,
    grad_slides,
    out_in,
    out_out,
    out_small,
    pads,
    gpad,
    taps,
    mixed,
    win,
    wout,
    normed,
    rstd,
    normal,
    act,
    slope,
    branch,
    upstream,
    gb_low,
    gnorm,
    gbias,
    mixed_bias,
    grads,
    from_core,
    from_dp,
    from_row,
    from_col,
    final,
    small,
    small_row,
    small_cd,
    small_out,
    row_send,
    col_send,
    cor_send,
    row_recv,
    col_recv,
    cor_recv,
    cor_wide,
    sem_local,
    sem_ws,
    sem_wr,
    sem_hs,
    sem_hr,
    sem_gs,
    sem_gr,
    sem_ss,
    sem_sr,
    sem_out,
):
    R, C, DP = sizes["row"], sizes["col"], sizes["dp"]
    CD = C * DP
    L, NT, _, T, D = wout.shape[0], wout.shape[1], 0, wout.shape[2], wout.shape[3]
    J = D // LANES
    H, W = slides.shape[1], slides.shape[2]
    N = H * W
    DH = D // DP
    UN = DH // UNIT
    row, col, dp = lax.axis_index("row"), lax.axis_index("col"), lax.axis_index("dp")
    cd = col * DP + dp
    core = row % 2

    def remote(src, dst, ssem, rsem, **where):
        return pltpu.make_async_remote_copy(
            src_ref=src,
            dst_ref=dst,
            send_sem=ssem,
            recv_sem=rsem,
            device_id=where,
            device_id_type=MESH,
        )

    def flip(index, bit):
        return index + bit - 2 * bit * ((index // bit) % 2)

    def there(dr, dc):
        ok = True
        if dr:
            ok = (row > 0) if dr < 0 else (row < R - 1)
        if dc:
            side = (col > 0) if dc < 0 else (col < C - 1)
            ok = side if ok is True else jnp.logical_and(ok, side)
        return ok

    def cd_peer(k):
        peer = (cd + k) % CD
        return peer, peer // DP, peer % DP

    barrier = pltpu.get_barrier_semaphore()
    for k in range(1, R):
        pl.semaphore_signal(
            barrier, inc=1, device_id={"row": (row + k) % R}, device_id_type=MESH
        )
    for k in range(1, CD):
        _, pc, pd = cd_peer(k)
        pl.semaphore_signal(
            barrier, inc=1, device_id={"col": pc, "dp": pd}, device_id_type=MESH
        )
    for dr, dc in DIAGONAL:

        @pl.when(there(dr, dc))
        def _():
            pl.semaphore_signal(
                barrier,
                inc=1,
                device_id={"row": row + dr, "col": col + dc},
                device_id_type=MESH,
            )

    own_in = [
        pltpu.make_async_copy(
            weight_in.at[l], win.at[l, pl.ds(dp * DH, DH), :], sem_local.at[l, 0]
        )
        for l in range(L)
    ]
    own_out = [
        pltpu.make_async_copy(
            weight_out.at[l],
            wout.at[l, :, :, pl.ds(dp * DH, DH)],
            sem_local.at[l, 1],
        )
        for l in range(L)
    ]
    for l in range(L):
        own_in[l].start()
        own_out[l].start()

    tall = H + 6
    zero_line = jnp.zeros((W + 2 * LEFT, LANES), F32)

    def clear(i, _):
        for j in range(J):
            for l in range(L):
                pads[l, j, i] = zero_line
            gpad[j, i] = zero_line
        return 0

    lax.fori_loop(0, tall, clear, 0)
    small[...] = jnp.zeros_like(small)
    for l in range(L):
        for p in range(7):
            for j in range(J):
                taps[l, j, 7 * p : 7 * p + 7, :] = kernel[
                    l, p, :, j * LANES : (j + 1) * LANES
                ]

    def fill(i, _):
        line = slides[0, i].astype(F32)
        for j in range(J):
            pads[0, j, i + 3, LEFT : LEFT + W, :] = line[:, j * LANES : (j + 1) * LANES]
        return 0

    lax.fori_loop(0, H, fill, 0)
    cor_wide[...] = jnp.zeros_like(cor_wide)

    def halo_copy(which, turn):
        if which < 4:
            dr, dc = STRAIGHT[which]
            if dr:
                src, dst = row_send.at[which], row_recv.at[turn, which]
            else:
                src, dst = col_send.at[which - 2], col_recv.at[turn, which - 2]
        else:
            dr, dc = DIAGONAL[which - 4]
            src, dst = cor_send.at[which - 4], cor_recv.at[turn, which - 4]
        where = {}
        if dr:
            where["row"] = row + dr
        if dc:
            where["col"] = col + dc
        return remote(src, dst, sem_hs.at[which], sem_hr.at[turn, which], **where)

    def lanes(j):
        return slice(j * LANES, (j + 1) * LANES)

    def halo_send(turn, src):
        for which, first in ((0, 3), (1, H)):
            for i in range(3):
                for j in range(J):
                    row_send[which, i, :, lanes(j)] = src[
                        j, first + i, LEFT : LEFT + W, :
                    ].astype(BF16)

            @pl.when(there(*STRAIGHT[which]))
            def _():
                halo_copy(which, turn).start()

        for which, first in ((2, LEFT), (3, LEFT + W - 3)):
            for i in range(3):
                for j in range(J):
                    col_send[which - 2, i, :, lanes(j)] = src[
                        j, 3 : 3 + H, first + i, :
                    ].astype(BF16)

            @pl.when(there(*STRAIGHT[which]))
            def _():
                halo_copy(which, turn).start()

        for k, (dr, dc) in enumerate(DIAGONAL):
            first, start = (3 if dr < 0 else H), (LEFT if dc < 0 else LEFT + W - 3)
            for i in range(3):
                for j in range(J):
                    cor_wide[3 * i : 3 * i + 3, lanes(j)] = src[
                        j, first + i, start : start + 3, :
                    ]
            cor_send[k] = cor_wide[...].astype(BF16)

            @pl.when(there(dr, dc))
            def _():
                halo_copy(4 + k, turn).start()

    def halo_recv(turn, dst):
        for which in (0, 1):
            first = H + 3 if which == 0 else 0
            dr, dc = STRAIGHT[which]

            @pl.when(there(-dr, -dc))
            def _():
                halo_copy(which, turn).wait_recv()
                for i in range(3):
                    line = row_recv[turn, which, i].astype(F32)
                    for j in range(J):
                        dst[j, first + i, LEFT : LEFT + W, :] = line[:, lanes(j)]

        for which in (2, 3):
            first = LEFT + W if which == 2 else LEFT - 3
            dr, dc = STRAIGHT[which]

            @pl.when(there(-dr, -dc))
            def _():
                halo_copy(which, turn).wait_recv()
                for i in range(3):
                    line = col_recv[turn, which - 2, i].astype(F32)
                    for j in range(J):
                        dst[j, 3 : 3 + H, first + i, :] = line[:, lanes(j)]

        for k, (dr, dc) in enumerate(DIAGONAL):
            first, start = (H + 3 if dr < 0 else 0), (LEFT + W if dc < 0 else LEFT - 3)

            @pl.when(there(-dr, -dc))
            def _():
                halo_copy(4 + k, turn).wait_recv()
                block = cor_recv[turn, k].astype(F32)
                for i in range(3):
                    for j in range(J):
                        dst[j, first + i, start : start + 3, :] = block[
                            3 * i : 3 * i + 3, lanes(j)
                        ]

        for which in range(8):
            dr, dc = (STRAIGHT + DIAGONAL)[which]

            @pl.when(there(dr, dc))
            def _():
                halo_copy(which, turn).wait_send()

    quarter = row % QUARTERS
    pieces = 2

    def held(which, l, p, side, q):
        if which == 0:
            rows = DH // QUARTERS // pieces
            return win.at[
                l, pl.ds(side * DH + (q * pieces + p) * rows, rows), :
            ]
        tiles = NT // QUARTERS // pieces
        return wout.at[
            l, pl.ds((q * pieces + p) * tiles, tiles), :, pl.ds(side * DH, DH)
        ]

    def own(which, l, p):
        if which == 0:
            rows = DH // QUARTERS // pieces
            return weight_in.at[l, pl.ds((quarter * pieces + p) * rows, rows), :]
        tiles = NT // QUARTERS // pieces
        return weight_out.at[l, pl.ds((quarter * pieces + p) * tiles, tiles)]

    other = 1 - dp

    def w_x(l, which, p):
        k = (l * 2 + which) * pieces + p
        return remote(
            own(which, l, p),
            held(which, l, p, dp, quarter),
            sem_ws.at[0, k],
            sem_wr.at[0, k],
            dp=1 - dp,
        )

    def w_hop(l, which, p, stage):
        k = (l * 2 + which) * pieces + p
        bit = 2 if stage == 1 else 1
        q = flip(quarter, 2) if stage == 3 else quarter
        part = held(which, l, p, other, q)
        return remote(
            part, part, sem_ws.at[stage, k], sem_wr.at[stage, k], row=flip(row, bit)
        )

    def weights_x(l, which):
        for p in range(pieces):
            w_x(l, which, p).start()

    def weights_forward(l, which):
        for p in range(pieces):
            w_x(l, which, p).wait()
            w_hop(l, which, p, 1).start()
            w_hop(l, which, p, 2).start()

    def weights_second(l, which):
        for p in range(pieces):
            w_hop(l, which, p, 1).wait()
            w_hop(l, which, p, 3).start()

    def weights_ready(l, which):
        for p in range(pieces):
            w_hop(l, which, p, 2).wait()
            w_hop(l, which, p, 3).wait()
        (own_in, own_out)[which][l].wait()

    def conv(src, l, mirrored, base, put):
        blocks = H // 8

        def one(index, _):
            j, start = index // blocks, (index % blocks) * 8
            totals = base(j, start)
            for q in range(7):
                for line in range(14):
                    window = src[
                        j, start + line, LEFT - 3 + q : LEFT - 3 + q + W, :
                    ]
                    for p in range(7):
                        i = line - p
                        if 0 <= i < 8:
                            k = 7 * p + q
                            k = 48 - k if mirrored else k
                            totals[i] = totals[i] + window * taps[l, j, k : k + 1, :]
            put(j, start, totals)
            return 0

        lax.fori_loop(0, J * blocks, one, 0)

    def tap_sums(l):
        for q in range(7):

            def lane_block(j, _):
                def block(index, totals):
                    start = index * 8
                    totals = list(totals)
                    for part in range(0, W, 8):
                        ups = [
                            gpad[j, start + 3 + i, LEFT + part : LEFT + part + 8, :]
                            for i in range(8)
                        ]
                        for line in range(14):
                            first = LEFT - 3 + part + q
                            window = pads[l, j, start + line, first : first + 8, :]
                            for p in range(7):
                                i = line - p
                                if 0 <= i < 8:
                                    totals[p] = totals[p] + window * ups[i]
                    return tuple(totals)

                zero = jnp.zeros((8, LANES), F32)
                totals = lax.fori_loop(0, H // 8, block, (zero,) * 7)
                for p in range(7):
                    put_small(
                        l, 7 * p + q, j, jnp.sum(totals[p], axis=0, keepdims=True)
                    )
                return 0

            lax.fori_loop(0, J, lane_block, 0)

    M = small.shape[3]

    def put_small(l, line, j, value):
        unit = (line // 8) * J + j
        small[
            l, unit // (CD * M), (unit // M) % CD, unit % M, line % 8 : line % 8 + 1, :
        ] = value

    def put_row(l, line, value):
        for j in range(J):
            put_small(l, line, j, value[:, lanes(j)])

    def forward(l, last):
        bias_line = kernel_bias[l : l + 1, :]

        for j in range(J):
            mixed_bias[j] = bias_line[:, lanes(j)]

        def base(j, start):
            del start
            bias = mixed_bias[j]
            return [jnp.broadcast_to(bias, (W, LANES)) for _ in range(8)]

        def put(j, start, totals):
            for i in range(8):
                mixed[j, start + i] = totals[i]

        conv(pads.at[l], l, False, base, put)
        gain, shift = norm_gain[l : l + 1, :], norm_bias[l : l + 1, :]

        def norm(i, _):
            lines = pl.ds(i * W, W)
            value = jnp.concatenate([mixed[j, i] for j in range(J)], axis=1)
            center = value - jnp.mean(value, -1, keepdims=True)
            scale = lax.rsqrt(jnp.mean(center * center, -1, keepdims=True) + EPSILON)
            out = center * scale
            normed[l, lines, :] = out
            rstd[l, lines, :] = scale
            normal[l, lines, :] = (out * gain + shift).astype(BF16)
            return 0

        lax.fori_loop(0, H, norm, 0)
        weights_second(l, 0)
        weights_ready(l, 0)

        def expand(t, _):
            cols = pl.ds(pl.multiple_of(t * T, T), T)
            hidden = jnp.dot(normal[l], win[l, :, cols], preferred_element_type=F32)
            hidden = hidden + bias_in[l : l + 1, cols]
            square = hidden * hidden
            tangent = jnp.tanh(hidden * (COEF + (COEF * CUBIC) * square))
            half = 0.5 * hidden
            both = 1.0 + tangent
            act[l, t] = (half * both).astype(BF16)
            slope[l, t] = 0.5 * both + half * (1.0 - tangent * tangent) * (
                COEF + (3.0 * COEF * CUBIC) * square
            )
            return 0

        lax.fori_loop(0, NT, expand, 0)
        weights_second(l, 1)
        weights_ready(l, 1)
        branch[l] = jnp.broadcast_to(bias_out[l : l + 1, :], (N, D))

        def project(t, _):
            branch[l] += jnp.dot(act[l, t], wout[l, t], preferred_element_type=F32)
            return 0

        lax.fori_loop(0, NT, project, 0)
        scales = layer_scale[l : l + 1, :]

        def finish(i, _):
            part = scales * branch[l, pl.ds(i * W, W), :]
            for j in range(J):
                old = pads[l, j, i + 3, LEFT : LEFT + W, :]
                new = (old + part[:, lanes(j)]).astype(BF16)
                if last:
                    output[0, i, :, lanes(j)] = new
                else:
                    pads[l + 1, j, i + 3, LEFT : LEFT + W, :] = new.astype(F32)
            return 0

        lax.fori_loop(0, H, finish, 0)

    bits = []
    bit = 2
    while bit < R:
        bits.append(bit)
        bit *= 2
    levels = []
    count = UN
    for b in bits:
        halve = count // 2 >= C
        levels.append((b, count, halve))
        count = count // 2 if halve else count
    left_units = count
    per_col = left_units // C
    nb = len(bits)
    S_CORE, S_DP, S_ROW, S_COL = 0, 1, 2, 2 + nb
    S_COLG = S_COL + C - 1
    S_ROWG = S_COLG + C - 1
    S_COREG = S_ROWG + nb

    def unit_base(level):
        start = 0
        for b, n, halve in levels[:level]:
            if halve:
                start = start + ((row // b) % 2) * (n // 2)
        return start

    def g_core(l, t):
        return remote(
            grads.at[l, t, 1 - core],
            from_core.at[l, t],
            sem_gs.at[t, S_CORE],
            sem_gr.at[l, t, S_CORE],
            row=flip(row, 1),
        )

    def g_dp(l, t):
        return remote(
            grads.at[l, t, core, 1 - dp],
            from_dp.at[l, t],
            sem_gs.at[t, S_DP],
            sem_gr.at[l, t, S_DP],
            dp=1 - dp,
        )

    row_slot = []
    at = 0
    for b, n, halve in levels:
        row_slot.append(at)
        at += n // 2 if halve else n

    def g_row(l, t, level):
        b, n, halve = levels[level]
        mine = (row // b) % 2
        start = unit_base(level)
        m = n
        if halve:
            m = n // 2
            start = start + (1 - mine) * m
        return remote(
            grads.at[l, t, core, dp, pl.ds(start, m)],
            from_row.at[l, t, pl.ds(row_slot[level], m)],
            sem_gs.at[t, S_ROW + level],
            sem_gr.at[l, t, S_ROW + level],
            row=flip(row, b),
        )

    def g_row_add(l, t, level):
        b, n, halve = levels[level]
        start = unit_base(level + 1)
        m = n // 2 if halve else n
        mine = grads.at[l, t, core, dp, pl.ds(start, m)]
        mine[...] = mine[...] + from_row[l, t, pl.ds(row_slot[level], m)]

    col_base = unit_base(nb)

    def g_col(l, t, k):
        peer = (col + k) % C
        return remote(
            grads.at[l, t, core, dp, pl.ds(col_base + peer * per_col, per_col)],
            from_col.at[l, t, k - 1],
            sem_gs.at[t, S_COL + k - 1],
            sem_gr.at[l, t, S_COL + k - 1],
            col=peer,
        )

    def g_colg(l, t, k):
        peer = (col + k) % C
        part = final.at[l, core, t, pl.ds(col_base + col * per_col, per_col)]
        return remote(
            part,
            part,
            sem_gs.at[t, S_COLG + k - 1],
            sem_gr.at[l, t, S_COLG + k - 1],
            col=peer,
        )

    def g_rowg(l, t, level):
        b, n, halve = levels[level]
        part = final.at[l, core, t, pl.ds(unit_base(level + 1), n // 2)]
        return remote(
            part,
            part,
            sem_gs.at[t, S_ROWG + level],
            sem_gr.at[l, t, S_ROWG + level],
            row=flip(row, b),
        )

    def g_coreg(l, t):
        part = final.at[l, core, t]
        return remote(
            part,
            part,
            sem_gs.at[t, S_COREG],
            sem_gr.at[l, t, S_COREG],
            row=flip(row, 1),
        )

    def go_dp(l, t):
        g_core(l, t).wait()
        mine = grads.at[l, t, core]
        mine[...] = mine[...] + from_core[l, t]
        g_dp(l, t).start()

    def go_row(l, t):
        g_dp(l, t).wait()
        mine = grads.at[l, t, core, dp]
        mine[...] = mine[...] + from_dp[l, t]
        for level in range(nb):
            if level:
                g_row(l, t, level - 1).wait()
                g_row_add(l, t, level - 1)
            g_row(l, t, level).start()

    def go_col(l, t):
        if nb:
            g_row(l, t, nb - 1).wait()
            g_row_add(l, t, nb - 1)
        for k in range(1, C):
            g_col(l, t, k).start()

    def go_colg(l, t):
        for k in range(1, C):
            g_col(l, t, k).wait()
        place = pl.ds(col_base + col * per_col, per_col)
        total = grads[l, t, core, dp, place].astype(F32)
        for k in range(1, C):
            total = total + from_col[l, t, k - 1].astype(F32)
        final[l, core, t, place] = total.astype(BF16)
        for k in range(1, C):
            g_colg(l, t, k).start()

    halved = [k for k in range(nb) if levels[k][2]][::-1]

    def go_rowg(l, t):
        for k in range(1, C):
            g_colg(l, t, k).wait()
        for n, level in enumerate(halved):
            if n:
                g_rowg(l, t, halved[n - 1]).wait()
            g_rowg(l, t, level).start()

    def go_coreg(l, t):
        if halved:
            g_rowg(l, t, halved[-1]).wait()
        g_coreg(l, t).start()

    def out_copies(l, t):
        cols = pl.ds(pl.multiple_of(t * T, T), T)
        return (
            pltpu.make_async_copy(
                final.at[l, 0, t], out_in.at[l, :, :, cols], sem_out.at[0, l, t]
            ),
            pltpu.make_async_copy(
                final.at[l, 1, t], out_out.at[l, t], sem_out.at[1, l, t]
            ),
        )

    def go_out(l, t):
        g_coreg(l, t).wait()
        for copy in out_copies(l, t):
            copy.start()

    chain = (go_row, go_col, go_colg, go_rowg, go_coreg, go_out)

    def tick(l, m):
        for behind, stage in enumerate(chain):
            t = m - behind
            if isinstance(m, int):
                if 0 <= t < NT:
                    stage(l, t)
            else:

                @pl.when(jnp.logical_and(t >= 0, t < NT))
                def _():
                    stage(l, t)

    ticks = NT + len(chain) - 1

    def run_ticks(l, first, end):
        def one(m, _):
            tick(l, m)
            return 0

        lax.fori_loop(first, end, one, 0)

    def s_copy(l, stage, k):
        if stage in (0, 3):
            peer = (row + k) % R
            where = {"row": peer}
        else:
            peer, pc, pd = cd_peer(k)
            where = {"col": pc, "dp": pd}
        if stage == 0:
            src, dst = small.at[l, peer], small_row.at[l, k - 1]
        elif stage == 1:
            src, dst = small.at[l, row, peer], small_cd.at[l, k - 1]
        elif stage == 2:
            src = dst = small_out.at[l, row, cd]
        else:
            src = dst = small_out.at[l, row]
        return remote(
            src, dst, sem_ss.at[stage, k - 1], sem_sr.at[l, stage, k - 1], **where
        )

    def small_start(l):
        for k in range(1, R):
            s_copy(l, 0, k).start()

    def small_second(l):
        for k in range(1, R):
            s_copy(l, 0, k).wait()
        total = small[l, row]
        for k in range(1, R):
            total = total + small_row[l, k - 1]
        small[l, row] = total
        for k in range(1, CD):
            s_copy(l, 1, k).start()

    def small_third(l):
        for k in range(1, CD):
            s_copy(l, 1, k).wait()
        total = small[l, row, cd]
        for k in range(1, CD):
            total = total + small_cd[l, k - 1]
        small_out[l, row, cd] = total
        for k in range(1, CD):
            s_copy(l, 2, k).start()

    def small_fourth(l):
        for k in range(1, CD):
            s_copy(l, 2, k).wait()
        for k in range(1, R):
            s_copy(l, 3, k).start()

    def small_end(l):
        for k in range(1, R):
            s_copy(l, 3, k).wait()

    def backward(l, turn, busy, last):
        scales = layer_scale[l : l + 1, :]
        empty = jnp.zeros((8, D), F32)

        def fold(value):
            total = value[0:8]
            for k in range(8, value.shape[0], 8):
                total = total + value[k : k + 8]
            return total

        def before(i, sums):
            lines = pl.ds(i * W, W)
            up = upstream[lines, :]
            gb = up * scales
            gb_low[lines, :] = gb.astype(BF16)
            return (sums[0] + fold(up * branch[l, lines, :]), sums[1] + fold(gb))

        sums = lax.fori_loop(0, H, before, (empty,) * 2)
        put_row(l, 53, jnp.sum(sums[0], 0, keepdims=True))
        put_row(l, 52, jnp.sum(sums[1], 0, keepdims=True))
        gnorm[...] = jnp.zeros_like(gnorm)

        def tile(t, _):
            cols = pl.ds(pl.multiple_of(t * T, T), T)
            gb = gb_low[...]
            ga = lax.dot_general(gb, wout[l, t], COLS, preferred_element_type=F32)
            gh = ga * slope[l, t]
            gbias[t] = jnp.sum(gh, 0, keepdims=True)
            low = gh.astype(BF16)
            g_out = lax.dot_general(act[l, t], gb, ROWS, preferred_element_type=F32)
            g_in = lax.dot_general(normal[l], low, ROWS, preferred_element_type=F32)
            for d in range(DP):
                grads[l, t, 0, d] = (
                    g_in[d * DH : (d + 1) * DH].astype(BF16).reshape(UN, UNIT, T)
                )
                grads[l, t, 1, d] = (
                    g_out[:, d * DH : (d + 1) * DH].astype(BF16).reshape(UN, UNIT, T)
                )
            g_core(l, t).start()
            gnorm[...] += lax.dot_general(
                low, win[l, :, cols], COLS, preferred_element_type=F32
            )

            @pl.when(t >= 2)
            def _():
                go_dp(l, t - 2)

            busy(t)
            return 0

        lax.fori_loop(0, NT, tile, 0)
        for t in range(NT - 2, NT):
            go_dp(l, t)
        per_line = D // T
        for t in range(NT):
            for half in range(T // LANES):
                j = (t % per_line) * (T // LANES) + half
                put_small(l, 54 + t // per_line, j, gbias[t, :, lanes(half)])
        gain = norm_gain[l : l + 1, :]

        def after(i, sums):
            lines = pl.ds(i * W, W)
            gn, unit = gnorm[lines, :], normed[l, lines, :]
            both = gn * unit
            gs = gn * gain
            first = jnp.mean(gs, -1, keepdims=True)
            second = jnp.mean(gs * unit, -1, keepdims=True)
            gm = rstd[l, lines, :] * (gs - first - unit * second)
            for j in range(J):
                gpad[j, i + 3, LEFT : LEFT + W, :] = gm[:, lanes(j)]
            return (sums[0] + fold(gm), sums[1] + fold(both), sums[2] + fold(gn))

        sums = lax.fori_loop(0, H, after, (empty,) * 3)
        for k in range(3):
            put_row(l, 49 + k, jnp.sum(sums[k], 0, keepdims=True))
        halo_send(turn, gpad)
        tap_sums(l)
        small_start(l)
        halo_recv(turn, gpad)

        def base(j, start):
            return [up_block[j, start + i] for i in range(8)]

        up_block = mixed

        def spread(i, _):
            for j in range(J):
                mixed[j, i] = upstream[pl.ds(i * W, W), lanes(j)]
            return 0

        lax.fori_loop(0, H, spread, 0)

        def put(j, start, totals):
            for i in range(8):
                mixed[j, start + i] = totals[i]

        small_second(l)
        conv(gpad, l, True, base, put)

        def gather(i, _):
            for j in range(J):
                if last:
                    grad_slides[0, i, :, lanes(j)] = mixed[j, i].astype(BF16)
                else:
                    upstream[pl.ds(i * W, W), lanes(j)] = mixed[j, i]
            return 0

        lax.fori_loop(0, H, gather, 0)

    diagonals = jnp.where(row > 0, 1, 0) + jnp.where(row < R - 1, 1, 0)
    diagonals = diagonals * (
        jnp.where(col > 0, 1, 0) + jnp.where(col < C - 1, 1, 0)
    )
    pl.semaphore_wait(barrier, R - 1 + CD - 1 + diagonals)
    halo_send(0, pads.at[0])
    for l in range(L):
        for which in range(2):
            weights_x(l, which)
    halo_recv(0, pads.at[0])

    def start_up(i, _):
        upstream[pl.ds(i * W, W), :] = cotangent[0, i].astype(F32)
        return 0

    lax.fori_loop(0, H, start_up, 0)
    weights_forward(0, 0)
    for l in range(L):
        if l:
            halo_recv(l, pads.at[l])
            weights_forward(l, 0)
        weights_forward(l, 1)
        forward(l, l == L - 1)
        if l + 1 < L:
            halo_send(l + 1, pads.at[l + 1])

    done = 0
    for n, l in enumerate(reversed(range(L))):
        if n == 0:
            backward(l, L + n, lambda t: None, l == 0)
        else:
            prior = l + 1

            def busy(t, prior=prior):
                @pl.when(t % 3 == 2)
                def _():
                    tick(prior, 1 + t // 3)

            run_ticks(prior, 0, 1)
            small_third(prior)
            backward(l, L + n, busy, l == 0)
            small_fourth(prior)
            done = 1 + NT // 3
            run_ticks(prior, done, ticks)
            small_end(prior)
    small_third(0)
    small_fourth(0)
    run_ticks(0, 0, ticks)
    small_end(0)
    for l in range(L):
        pltpu.sync_copy(small_out.at[l], out_small.at[l])

    def drain(t, _):
        for l in range(L):
            for copy in out_copies(l, t):
                copy.wait()
        return 0

    lax.fori_loop(0, NT, drain, 0)


def per_device(
    sizes,
    slides,
    cotangent,
    kernel,
    kernel_bias,
    norm_gain,
    norm_bias,
    weight_in,
    bias_in,
    weight_out,
    bias_out,
    layer_scale,
):
    R, C, DP = sizes["row"], sizes["col"], sizes["dp"]
    CD = C * DP
    L, DH, FF = weight_in.shape
    D = slides.shape[-1]
    H, W = slides.shape[1], slides.shape[2]
    N = H * W
    J = D // LANES
    T = DH
    NT = FF // T
    UN = DH // UNIT
    everyone = R * CD
    need = -(-(54 + FF // D) // 8) * J
    M = -(-need // everyone)
    row_units, count, bit, nb = 0, UN, 2, 0
    while bit < R:
        halve = count // 2 >= C
        count = count // 2 if halve else count
        row_units += count
        bit *= 2
        nb += 1
    per_col = count // C
    stages = 2 + nb + 2 * (C - 1) + nb + 1
    small_peers = max(R, CD) - 1
    vmem = pl.BlockSpec(memory_space=pltpu.VMEM)
    hbm = pl.BlockSpec(memory_space=pl.ANY)
    V = pltpu.VMEM
    DMA = pltpu.SemaphoreType.DMA
    turns = 2 * L
    out = pl.pallas_call(
        functools.partial(step_body, sizes),
        out_shape=(
            jax.ShapeDtypeStruct((1, H, W, D), BF16),
            jax.ShapeDtypeStruct((1, H, W, D), BF16),
            jax.ShapeDtypeStruct((L, UN, UNIT, FF), BF16),
            jax.ShapeDtypeStruct((L, NT, UN, UNIT, DH), BF16),
            jax.ShapeDtypeStruct((L, R, CD, M, 8, LANES), F32),
        ),
        in_specs=[vmem] * 6 + [hbm, vmem, hbm, vmem, vmem],
        out_specs=(vmem, vmem, hbm, hbm, hbm),
        scratch_shapes=[
            V((L, J, H + 6, W + 2 * LEFT, LANES), F32),
            V((J, H + 6, W + 2 * LEFT, LANES), F32),
            V((L, J, 49, LANES), F32),
            V((J, H, W, LANES), F32),
            V((L, D, FF), BF16),
            V((L, NT, T, D), BF16),
            V((L, N, D), F32),
            V((L, N, 1), F32),
            V((L, N, D), BF16),
            V((L, NT, N, T), BF16),
            V((L, NT, N, T), F32),
            V((L, N, D), F32),
            V((N, D), F32),
            V((N, D), BF16),
            V((N, D), F32),
            V((NT, 1, T), F32),
            V((J, 1, LANES), F32),
            V((L, NT, 2, DP, UN, UNIT, T), BF16),
            V((L, NT, DP, UN, UNIT, T), BF16),
            V((L, NT, UN, UNIT, T), BF16),
            V((L, NT, max(row_units, 1), UNIT, T), BF16),
            V((L, NT, max(C - 1, 1), per_col, UNIT, T), BF16),
            V((L, 2, NT, UN, UNIT, T), BF16),
            V((L, R, CD, M, 8, LANES), F32),
            V((L, max(R - 1, 1), CD, M, 8, LANES), F32),
            V((L, max(CD - 1, 1), M, 8, LANES), F32),
            V((L, R, CD, M, 8, LANES), F32),
            V((2, 3, W, D), BF16),
            V((2, 3, H, D), BF16),
            V((4, UNIT, D), BF16),
            V((turns, 2, 3, W, D), BF16),
            V((turns, 2, 3, H, D), BF16),
            V((turns, 4, UNIT, D), BF16),
            V((UNIT, D), F32),
            DMA((L, 2)),
            DMA((4, 4 * L)),
            DMA((4, 4 * L)),
            DMA((8,)),
            DMA((turns, 8)),
            DMA((NT, stages)),
            DMA((L, NT, stages)),
            DMA((4, small_peers)),
            DMA((L, 4, small_peers)),
            DMA((2, L, NT)),
        ],
        compiler_params=pltpu.CompilerParams(
            collective_id=0, has_side_effects=True, vmem_limit_bytes=67043328
        ),
        name="step",
    )(
        slides,
        cotangent,
        kernel,
        kernel_bias,
        norm_gain,
        norm_bias,
        weight_in,
        bias_in,
        weight_out.reshape(L, NT, T, DH),
        bias_out,
        layer_scale,
    )
    output, grad_slides, low_in, low_out, small = out
    lines = small.reshape(L, -1, J, 8, LANES).transpose(0, 1, 3, 2, 4)
    lines = lines.reshape(L, -1, D)
    return (
        output,
        grad_slides,
        low_in.reshape(L, DH, FF).astype(F32),
        low_out.reshape(L, FF, DH).astype(F32),
        lines[:, :49].reshape(L, 7, 7, D),
        lines[:, 49:54],
        lines[:, 54 : 54 + FF // D].reshape(L, FF),
    )


def solution(mesh):
    return jax.shard_map(
        functools.partial(per_device, dict(mesh.shape)),
        mesh=mesh,
        in_specs=(
            P("dp", "row", "col", None),
            P("dp", "row", "col", None),
            P(),
            P(),
            P(),
            P(),
            P(None, "dp", None),
            P(),
            P(None, None, "dp"),
            P(),
            P(),
        ),
        out_specs=(
            P("dp", "row", "col", None),
            P("dp", "row", "col", None),
            P(None, "dp", None),
            P(None, None, "dp"),
            P(),
            P(),
            P(),
        ),
        check_vma=False,
    )
```

```python
import functools

import jax
import jax.numpy as jnp
from jax import lax
from jax.experimental import pallas as pl
from jax.experimental.pallas import tpu as pltpu
from jax.sharding import PartitionSpec as P

COEF = 0.7978845608028654
CUBIC = 0.044715
EPSILON = 1e-06
LANES = 128
UNIT = 16
LEFT = 8
QUARTERS = 4
MESH = pl.DeviceIdType.MESH
F32 = jnp.float32
BF16 = jnp.bfloat16
STRAIGHT = ((-1, 0), (1, 0), (0, -1), (0, 1))
DIAGONAL = ((-1, -1), (-1, 1), (1, -1), (1, 1))
COLS = (((1,), (1,)), ((), ()))


def step_body(
    sizes,
    slides,
    cotangent,
    kernel,
    kernel_bias,
    norm_gain,
    norm_bias,
    weight_in,
    bias_in,
    weight_out,
    bias_out,
    layer_scale,
    output,
    grad_slides,
    out_in,
    out_out,
    out_small,
    pads,
    gpads,
    taps,
    mixed,
    win,
    wout,
    normed,
    rstd,
    normal,
    normal_t,
    act,
    slope,
    branch,
    upstream,
    gb_low,
    gb_t,
    gnorm,
    gbias,
    mixed_bias,
    grads,
    from_core,
    from_dp,
    from_row,
    from_col,
    final,
    small,
    small_row,
    small_cd,
    small_out,
    row_send,
    col_send,
    cor_send,
    row_recv,
    col_recv,
    cor_recv,
    cor_wide,
    sem_local,
    sem_ws,
    sem_wr,
    sem_hs,
    sem_hr,
    sem_gs,
    sem_gr,
    sem_ss,
    sem_sr,
    sem_out,
):
    R, C, DP = sizes["row"], sizes["col"], sizes["dp"]
    CD = C * DP
    L, NT, _, T, D = wout.shape[0], wout.shape[1], 0, wout.shape[2], wout.shape[3]
    J = D // LANES
    H, W = slides.shape[1], slides.shape[2]
    N = H * W
    DH = D // DP
    UN = DH // UNIT
    row, col, dp = lax.axis_index("row"), lax.axis_index("col"), lax.axis_index("dp")
    cd = col * DP + dp
    core = row % 2

    def remote(src, dst, ssem, rsem, **where):
        return pltpu.make_async_remote_copy(
            src_ref=src,
            dst_ref=dst,
            send_sem=ssem,
            recv_sem=rsem,
            device_id=where,
            device_id_type=MESH,
        )

    def flip(index, bit):
        return index + bit - 2 * bit * ((index // bit) % 2)

    def there(dr, dc):
        ok = True
        if dr:
            ok = (row > 0) if dr < 0 else (row < R - 1)
        if dc:
            side = (col > 0) if dc < 0 else (col < C - 1)
            ok = side if ok is True else jnp.logical_and(ok, side)
        return ok

    def cd_peer(k):
        peer = (cd + k) % CD
        return peer, peer // DP, peer % DP

    barrier = pltpu.get_barrier_semaphore()
    for k in range(1, R):
        pl.semaphore_signal(
            barrier, inc=1, device_id={"row": (row + k) % R}, device_id_type=MESH
        )
    for k in range(1, CD):
        _, pc, pd = cd_peer(k)
        pl.semaphore_signal(
            barrier, inc=1, device_id={"col": pc, "dp": pd}, device_id_type=MESH
        )
    for dr, dc in DIAGONAL:

        @pl.when(there(dr, dc))
        def _():
            pl.semaphore_signal(
                barrier,
                inc=1,
                device_id={"row": row + dr, "col": col + dc},
                device_id_type=MESH,
            )

    own_in = [
        pltpu.make_async_copy(
            weight_in.at[l], win.at[l, pl.ds(dp * DH, DH), :], sem_local.at[l, 0]
        )
        for l in range(L)
    ]
    own_out = [
        pltpu.make_async_copy(
            weight_out.at[l],
            wout.at[l, :, :, pl.ds(dp * DH, DH)],
            sem_local.at[l, 1],
        )
        for l in range(L)
    ]
    for l in range(L):
        own_in[l].start()
        own_out[l].start()

    tall = H + 6
    zero_line = jnp.zeros((W + 2 * LEFT, LANES), F32)

    def clear(i, _):
        for j in range(J):
            for l in range(L):
                pads[l, j, i] = zero_line
                gpads[l, j, i] = zero_line
        return 0

    lax.fori_loop(0, tall, clear, 0)
    small[...] = jnp.zeros_like(small)
    for l in range(L):
        for p in range(7):
            for j in range(J):
                for q in range(7):
                    taps[l, j, 7 * p + q : 7 * p + q + 1, :] = kernel[
                        p, q, l : l + 1, j * LANES : (j + 1) * LANES
                    ]

    def fill(i, _):
        line = slides[0, i].astype(F32)
        for j in range(J):
            pads[0, j, i + 3, LEFT : LEFT + W, :] = line[:, j * LANES : (j + 1) * LANES]
        return 0

    lax.fori_loop(0, H, fill, 0)
    cor_wide[...] = jnp.zeros_like(cor_wide)

    def halo_copy(which, turn):
        if which < 4:
            dr, dc = STRAIGHT[which]
            if dr:
                src, dst = row_send.at[which], row_recv.at[turn, which]
            else:
                src, dst = col_send.at[which - 2], col_recv.at[turn, which - 2]
        else:
            dr, dc = DIAGONAL[which - 4]
            src, dst = cor_send.at[which - 4], cor_recv.at[turn, which - 4]
        where = {}
        if dr:
            where["row"] = row + dr
        if dc:
            where["col"] = col + dc
        return remote(src, dst, sem_hs.at[which], sem_hr.at[turn, which], **where)

    def lanes(j):
        return slice(j * LANES, (j + 1) * LANES)

    def halo_send(turn, src):
        for which, first in ((0, 3), (1, H)):
            for i in range(3):
                for j in range(J):
                    row_send[which, i, :, lanes(j)] = src[
                        j, first + i, LEFT : LEFT + W, :
                    ].astype(BF16)

            @pl.when(there(*STRAIGHT[which]))
            def _():
                halo_copy(which, turn).start()

        for which, first in ((2, LEFT), (3, LEFT + W - 3)):
            for i in range(3):
                for j in range(J):
                    col_send[which - 2, i, :, lanes(j)] = src[
                        j, 3 : 3 + H, first + i, :
                    ].astype(BF16)

            @pl.when(there(*STRAIGHT[which]))
            def _():
                halo_copy(which, turn).start()

        for k, (dr, dc) in enumerate(DIAGONAL):
            first, start = (3 if dr < 0 else H), (LEFT if dc < 0 else LEFT + W - 3)
            for i in range(3):
                for j in range(J):
                    cor_wide[3 * i : 3 * i + 3, lanes(j)] = src[
                        j, first + i, start : start + 3, :
                    ]
            cor_send[k] = cor_wide[...].astype(BF16)

            @pl.when(there(dr, dc))
            def _():
                halo_copy(4 + k, turn).start()

    def halo_recv(turn, dst):
        for which in (0, 1):
            first = H + 3 if which == 0 else 0
            dr, dc = STRAIGHT[which]

            @pl.when(there(-dr, -dc))
            def _():
                halo_copy(which, turn).wait_recv()
                for i in range(3):
                    line = row_recv[turn, which, i].astype(F32)
                    for j in range(J):
                        dst[j, first + i, LEFT : LEFT + W, :] = line[:, lanes(j)]

        for which in (2, 3):
            first = LEFT + W if which == 2 else LEFT - 3
            dr, dc = STRAIGHT[which]

            @pl.when(there(-dr, -dc))
            def _():
                halo_copy(which, turn).wait_recv()
                for i in range(3):
                    line = col_recv[turn, which - 2, i].astype(F32)
                    for j in range(J):
                        dst[j, 3 : 3 + H, first + i, :] = line[:, lanes(j)]

        for k, (dr, dc) in enumerate(DIAGONAL):
            first, start = (H + 3 if dr < 0 else 0), (LEFT + W if dc < 0 else LEFT - 3)

            @pl.when(there(-dr, -dc))
            def _():
                halo_copy(4 + k, turn).wait_recv()
                block = cor_recv[turn, k].astype(F32)
                for i in range(3):
                    for j in range(J):
                        dst[j, first + i, start : start + 3, :] = block[
                            3 * i : 3 * i + 3, lanes(j)
                        ]

        for which in range(8):
            dr, dc = (STRAIGHT + DIAGONAL)[which]

            @pl.when(there(dr, dc))
            def _():
                halo_copy(which, turn).wait_send()

    quarter = row % QUARTERS
    pieces = NT // QUARTERS

    def held(which, l, p, side, q):
        t = q * pieces + p
        if which == 0:
            cols = pl.ds(pl.multiple_of(t * T, T), T)
            return win.at[l, pl.ds(side * DH, DH), cols]
        return wout.at[l, t, :, pl.ds(side * DH, DH)]

    def own(which, l, p):
        t = quarter * pieces + p
        if which == 0:
            return weight_in.at[l, :, pl.ds(pl.multiple_of(t * T, T), T)]
        return weight_out.at[l, t]

    other = 1 - dp

    def w_x(l, which, p):
        k = (l * 2 + which) * pieces + p
        return remote(
            own(which, l, p),
            held(which, l, p, dp, quarter),
            sem_ws.at[0, k],
            sem_wr.at[0, k],
            dp=1 - dp,
        )

    def w_hop(l, which, p, stage):
        k = (l * 2 + which) * pieces + p
        bit = 2 if stage == 1 else 1
        q = flip(quarter, 2) if stage == 3 else quarter
        part = held(which, l, p, other, q)
        return remote(
            part, part, sem_ws.at[stage, k], sem_wr.at[stage, k], row=flip(row, bit)
        )

    def weights_x(l, which):
        for p in range(pieces):
            w_x(l, which, p).start()

    def weights_forward(l, which, p):
        w_x(l, which, p).wait()
        w_hop(l, which, p, 1).start()
        w_hop(l, which, p, 2).start()

    def weights_second(l, which, p):
        w_hop(l, which, p, 1).wait()
        w_hop(l, which, p, 3).start()

    def weights_got(l, which, p, stage):
        w_hop(l, which, p, stage).wait()

    def my_tile(s):
        q, p = s // pieces, s % pieces
        spot = flip(quarter, 1) * (q % 2) + quarter * (1 - q % 2)
        return ((spot + 2 * (q // 2)) % QUARTERS) * pieces + p

    def conv(src, l, mirrored, base, put, during=None):
        blocks = H // 8

        def one(index, _):
            j, start = index // blocks, (index % blocks) * 8
            totals = base(j, start)
            for q in range(7):
                for line in range(14):
                    window = src[
                        j, start + line, LEFT - 3 + q : LEFT - 3 + q + W, :
                    ]
                    for p in range(7):
                        i = line - p
                        if 0 <= i < 8:
                            k = 7 * p + q
                            k = 48 - k if mirrored else k
                            totals[i] = totals[i] + window * taps[l, j, k : k + 1, :]
            put(j, start, totals)
            if during is not None:
                during(index)
            return 0

        lax.fori_loop(0, J * blocks, one, 0)

    def tap_sums(l, first, end, during):
        for q in range(first, end):

            def lane_block(j, _):
                def block(index, totals):
                    start = index * 8
                    totals = list(totals)
                    for part in range(0, W, 8):
                        ups = [
                            gpads[
                                l, j, start + 3 + i, LEFT + part : LEFT + part + 8, :
                            ]
                            for i in range(8)
                        ]
                        for line in range(14):
                            first = LEFT - 3 + part + q
                            window = pads[l, j, start + line, first : first + 8, :]
                            for p in range(7):
                                i = line - p
                                if 0 <= i < 8:
                                    totals[p] = totals[p] + window * ups[i]
                    return tuple(totals)

                zero = jnp.zeros((8, LANES), F32)
                totals = lax.fori_loop(0, H // 8, block, (zero,) * 7)
                for p in range(7):
                    put_small(
                        l, 7 * p + q, j, jnp.sum(totals[p], axis=0, keepdims=True)
                    )
                return 0

            lax.fori_loop(0, J, lane_block, 0)
            during(q)

    M = small.shape[3]

    def put_small(l, line, j, value):
        unit = (line // 8) * J + j
        small[
            l, unit // (CD * M), (unit // M) % CD, unit % M, line % 8 : line % 8 + 1, :
        ] = value

    def put_row(l, line, value):
        for j in range(J):
            put_small(l, line, j, value[:, lanes(j)])

    def transpose(src, dst):
        for k in range(N // LANES):
            block = src[k * LANES : (k + 1) * LANES, :].astype(F32)
            dst[:, lanes(k)] = block.T.astype(BF16)

    def forward(l, last, hooks):
        bias_line = kernel_bias[l : l + 1, :]
        for j in range(J):
            mixed_bias[j] = bias_line[:, lanes(j)]

        def base(j, start):
            del start
            bias = mixed_bias[j]
            return [jnp.broadcast_to(bias, (W, LANES)) for _ in range(8)]

        def put(j, start, totals):
            for i in range(8):
                mixed[j, start + i] = totals[i]

        conv(pads.at[l], l, False, base, put, hooks["conv"])
        hooks["conv"](-1)
        gain, shift = norm_gain[l : l + 1, :], norm_bias[l : l + 1, :]

        def norm(i, _):
            lines = pl.ds(i * W, W)
            value = jnp.concatenate([mixed[j, i] for j in range(J)], axis=1)
            center = value - jnp.mean(value, -1, keepdims=True)
            scale = lax.rsqrt(jnp.mean(center * center, -1, keepdims=True) + EPSILON)
            out = center * scale
            normed[l, lines, :] = out
            rstd[l, lines, :] = scale
            normal[l, lines, :] = (out * gain + shift).astype(BF16)
            return 0

        lax.fori_loop(0, H, norm, 0, unroll=4)
        hooks["norm"]()
        transpose(normal.at[l], normal_t.at[l])

        def expand(s, _):
            hooks["expand"](s)
            t = my_tile(s)
            cols = pl.ds(pl.multiple_of(t * T, T), T)
            hidden = jnp.dot(normal[l], win[l, :, cols], preferred_element_type=F32)
            hidden = hidden + bias_in[l : l + 1, cols]
            square = hidden * hidden
            tangent = jnp.tanh(hidden * (COEF + (COEF * CUBIC) * square))
            half = 0.5 * hidden
            both = 1.0 + tangent
            act[l, t] = (half * both).astype(BF16)
            rise = 0.5 * both + half * (1.0 - tangent * tangent) * (
                COEF + (3.0 * COEF * CUBIC) * square
            )
            slope[l, t] = rise.astype(BF16)
            return 0

        lax.fori_loop(0, NT, expand, 0)
        branch[l] = jnp.broadcast_to(bias_out[l : l + 1, :], (N, D))

        def project(s, _):
            hooks["project"](s)
            total = branch[l]
            for p in range(pieces):
                t = my_tile(s * pieces + p)
                total = total + jnp.dot(
                    act[l, t], wout[l, t], preferred_element_type=F32
                )
            branch[l] = total
            return 0

        lax.fori_loop(0, QUARTERS, project, 0)
        scales = layer_scale[l : l + 1, :]

        def finish(i, _):
            part = scales * branch[l, pl.ds(i * W, W), :]
            for j in range(J):
                old = pads[l, j, i + 3, LEFT : LEFT + W, :]
                new = (old + part[:, lanes(j)]).astype(BF16)
                if last:
                    output[0, i, :, lanes(j)] = new
                else:
                    pads[l + 1, j, i + 3, LEFT : LEFT + W, :] = new.astype(F32)
            return 0

        lax.fori_loop(0, H, finish, 0)

    bits = []
    bit = 2
    while bit < R:
        bits.append(bit)
        bit *= 2
    levels = []
    count = UN
    for b in bits:
        halve = count // 2 >= C
        levels.append((b, count, halve))
        count = count // 2 if halve else count
    left_units = count
    per_col = left_units // C
    nb = len(bits)
    S_CORE, S_DP, S_ROW, S_COL = 0, 1, 2, 2 + nb
    S_COLG = S_COL + C - 1
    S_ROWG = S_COLG + C - 1
    S_COREG = S_ROWG + nb

    def unit_base(level):
        start = 0
        for b, n, halve in levels[:level]:
            if halve:
                start = start + ((row // b) % 2) * (n // 2)
        return start

    def g_core(l, t):
        return remote(
            grads.at[l, t, 1 - core],
            from_core.at[l, t],
            sem_gs.at[t, S_CORE],
            sem_gr.at[l, t, S_CORE],
            row=flip(row, 1),
        )

    def g_dp(l, t):
        return remote(
            grads.at[l, t, core, 1 - dp],
            from_dp.at[l, t],
            sem_gs.at[t, S_DP],
            sem_gr.at[l, t, S_DP],
            dp=1 - dp,
        )

    row_slot = []
    at = 0
    for b, n, halve in levels:
        row_slot.append(at)
        at += n // 2 if halve else n

    def g_row(l, t, level):
        b, n, halve = levels[level]
        mine = (row // b) % 2
        start = unit_base(level)
        m = n
        if halve:
            m = n // 2
            start = start + (1 - mine) * m
        return remote(
            grads.at[l, t, core, dp, pl.ds(start, m)],
            from_row.at[l, t, pl.ds(row_slot[level], m)],
            sem_gs.at[t, S_ROW + level],
            sem_gr.at[l, t, S_ROW + level],
            row=flip(row, b),
        )

    def g_row_add(l, t, level):
        b, n, halve = levels[level]
        start = unit_base(level + 1)
        m = n // 2 if halve else n
        mine = grads.at[l, t, core, dp, pl.ds(start, m)]
        mine[...] = mine[...] + from_row[l, t, pl.ds(row_slot[level], m)]

    col_base = unit_base(nb)

    def g_col(l, t, k):
        peer = (col + k) % C
        return remote(
            grads.at[l, t, core, dp, pl.ds(col_base + peer * per_col, per_col)],
            from_col.at[l, t, k - 1],
            sem_gs.at[t, S_COL + k - 1],
            sem_gr.at[l, t, S_COL + k - 1],
            col=peer,
        )

    def g_colg(l, t, k):
        peer = (col + k) % C
        part = final.at[l, core, t, pl.ds(col_base + col * per_col, per_col)]
        return remote(
            part,
            part,
            sem_gs.at[t, S_COLG + k - 1],
            sem_gr.at[l, t, S_COLG + k - 1],
            col=peer,
        )

    def g_rowg(l, t, level):
        b, n, halve = levels[level]
        part = final.at[l, core, t, pl.ds(unit_base(level + 1), n // 2)]
        return remote(
            part,
            part,
            sem_gs.at[t, S_ROWG + level],
            sem_gr.at[l, t, S_ROWG + level],
            row=flip(row, b),
        )

    def g_coreg(l, t):
        part = final.at[l, core, t]
        return remote(
            part,
            part,
            sem_gs.at[t, S_COREG],
            sem_gr.at[l, t, S_COREG],
            row=flip(row, 1),
        )

    def go_dp(l, t):
        g_core(l, t).wait()
        mine = grads.at[l, t, core]
        mine[...] = mine[...] + from_core[l, t]
        g_dp(l, t).start()

    def go_row(l, t):
        g_dp(l, t).wait()
        mine = grads.at[l, t, core, dp]
        mine[...] = mine[...] + from_dp[l, t]
        for level in range(nb):
            if level:
                g_row(l, t, level - 1).wait()
                g_row_add(l, t, level - 1)
            g_row(l, t, level).start()

    def go_col(l, t):
        if nb:
            g_row(l, t, nb - 1).wait()
            g_row_add(l, t, nb - 1)
        for k in range(1, C):
            g_col(l, t, k).start()

    def go_colg(l, t):
        for k in range(1, C):
            g_col(l, t, k).wait()
        place = pl.ds(col_base + col * per_col, per_col)
        total = grads[l, t, core, dp, place].astype(F32)
        for k in range(1, C):
            total = total + from_col[l, t, k - 1].astype(F32)
        final[l, core, t, place] = total.astype(BF16)
        for k in range(1, C):
            g_colg(l, t, k).start()

    halved = [k for k in range(nb) if levels[k][2]][::-1]

    def go_rowg(l, t):
        for k in range(1, C):
            g_colg(l, t, k).wait()
        for n, level in enumerate(halved):
            if n:
                g_rowg(l, t, halved[n - 1]).wait()
            g_rowg(l, t, level).start()

    def go_coreg(l, t):
        if halved:
            g_rowg(l, t, halved[-1]).wait()
        g_coreg(l, t).start()

    def out_copies(l, t):
        cols = pl.ds(pl.multiple_of(t * T, T), T)
        return (
            pltpu.make_async_copy(
                final.at[l, 0, t], out_in.at[l, :, :, cols], sem_out.at[0, l, t]
            ),
            pltpu.make_async_copy(
                final.at[l, 1, t], out_out.at[l, :, :, cols], sem_out.at[1, l, t]
            ),
        )

    def go_out(l, t):
        g_coreg(l, t).wait()
        for copy in out_copies(l, t):
            copy.start()

    chain = (go_row, go_col, go_colg, go_rowg, go_coreg, go_out)

    def s_copy(l, stage, k):
        if stage in (0, 3):
            peer = (row + k) % R
            where = {"row": peer}
        else:
            peer, pc, pd = cd_peer(k)
            where = {"col": pc, "dp": pd}
        if stage == 0:
            src, dst = small.at[l, peer], small_row.at[l, k - 1]
        elif stage == 1:
            src, dst = small.at[l, row, peer], small_cd.at[l, k - 1]
        elif stage == 2:
            src = dst = small_out.at[l, row, cd]
        else:
            src = dst = small_out.at[l, row]
        return remote(
            src, dst, sem_ss.at[stage, k - 1], sem_sr.at[l, stage, k - 1], **where
        )

    def small_start(l):
        for k in range(1, R):
            s_copy(l, 0, k).start()

    def small_second(l):
        for k in range(1, R):
            s_copy(l, 0, k).wait()
        total = small[l, row]
        for k in range(1, R):
            total = total + small_row[l, k - 1]
        small[l, row] = total
        for k in range(1, CD):
            s_copy(l, 1, k).start()

    def small_third(l):
        for k in range(1, CD):
            s_copy(l, 1, k).wait()
        total = small[l, row, cd]
        for k in range(1, CD):
            total = total + small_cd[l, k - 1]
        small_out[l, row, cd] = total
        for k in range(1, CD):
            s_copy(l, 2, k).start()

    def small_fourth(l):
        for k in range(1, CD):
            s_copy(l, 2, k).wait()
        for k in range(1, R):
            s_copy(l, 3, k).start()

    def small_end(l):
        for k in range(1, R):
            s_copy(l, 3, k).wait()

    def backward(l, turn, hooks, last):
        gpad = gpads.at[l]
        scales = layer_scale[l : l + 1, :]
        empty = jnp.zeros((8, D), F32)

        def fold(value):
            total = value[0:8]
            for k in range(8, value.shape[0], 8):
                total = total + value[k : k + 8]
            return total

        def before(i, sums):
            lines = pl.ds(i * W, W)
            up = upstream[lines, :]
            gb = up * scales
            gb_low[lines, :] = gb.astype(BF16)
            return (sums[0] + fold(up * branch[l, lines, :]), sums[1] + fold(gb))

        sums = lax.fori_loop(0, H, before, (empty,) * 2)
        put_row(l, 53, jnp.sum(sums[0], 0, keepdims=True))
        put_row(l, 52, jnp.sum(sums[1], 0, keepdims=True))
        gnorm[...] = jnp.zeros_like(gnorm)
        transpose(gb_low, gb_t)

        def tile(t, _):
            cols = pl.ds(pl.multiple_of(t * T, T), T)
            gb = gb_low[...]
            ga = lax.dot_general(gb, wout[l, t], COLS, preferred_element_type=F32)
            gh = ga * slope[l, t].astype(F32)
            gbias[t] = jnp.sum(gh, 0, keepdims=True)
            low = gh.astype(BF16)
            g_out = jnp.dot(gb_t[...], act[l, t], preferred_element_type=F32)
            g_in = jnp.dot(normal_t[l], low, preferred_element_type=F32)
            for d in range(DP):
                grads[l, t, 0, d] = (
                    g_in[d * DH : (d + 1) * DH].astype(BF16).reshape(UN, UNIT, T)
                )
                grads[l, t, 1, d] = (
                    g_out[d * DH : (d + 1) * DH].astype(BF16).reshape(UN, UNIT, T)
                )
            g_core(l, t).start()
            gnorm[...] += lax.dot_general(
                low, win[l, :, cols], COLS, preferred_element_type=F32
            )

            @pl.when(t >= 2)
            def _():
                go_dp(l, t - 2)

            hooks('tile', t)
            return 0

        lax.fori_loop(0, NT, tile, 0)
        for t in range(NT - 2, NT):
            go_dp(l, t)
        hooks('rest', -1)
        per_line = D // T
        for t in range(NT):
            for half in range(T // LANES):
                j = (t % per_line) * (T // LANES) + half
                put_small(l, 54 + t // per_line, j, gbias[t, :, lanes(half)])
        gain = norm_gain[l : l + 1, :]

        def after(i, sums):
            lines = pl.ds(i * W, W)
            gn, unit = gnorm[lines, :], normed[l, lines, :]
            both = gn * unit
            gs = gn * gain
            first = jnp.mean(gs, -1, keepdims=True)
            second = jnp.mean(gs * unit, -1, keepdims=True)
            gm = rstd[l, lines, :] * (gs - first - unit * second)
            for j in range(J):
                gpad[j, i + 3, LEFT : LEFT + W, :] = gm[:, lanes(j)]
            return (sums[0] + fold(gm), sums[1] + fold(both), sums[2] + fold(gn))

        sums = lax.fori_loop(0, H, after, (empty,) * 3, unroll=2)
        for k in range(3):
            put_row(l, 49 + k, jnp.sum(sums[k], 0, keepdims=True))
        halo_send(turn, gpad)
        hooks('sent', -1)
        halo_recv(turn, gpad)

        def base(j, start):
            return [up_block[j, start + i] for i in range(8)]

        up_block = mixed

        def spread(i, _):
            for j in range(J):
                mixed[j, i] = upstream[pl.ds(i * W, W), lanes(j)]
            return 0

        lax.fori_loop(0, H, spread, 0)

        def put(j, start, totals):
            for i in range(8):
                mixed[j, start + i] = totals[i]

        conv(gpad, l, True, base, put, lambda k: hooks('conv', k))

        def gather(i, _):
            for j in range(J):
                if last:
                    grad_slides[0, i, :, lanes(j)] = mixed[j, i].astype(BF16)
                else:
                    upstream[pl.ds(i * W, W), lanes(j)] = mixed[j, i]
            return 0

        lax.fori_loop(0, H, gather, 0)

    diagonals = jnp.where(row > 0, 1, 0) + jnp.where(row < R - 1, 1, 0)
    diagonals = diagonals * (
        jnp.where(col > 0, 1, 0) + jnp.where(col < C - 1, 1, 0)
    )
    pl.semaphore_wait(barrier, R - 1 + CD - 1 + diagonals)
    halo_send(0, pads.at[0])
    for l in range(L):
        for which in range(2):
            weights_x(l, which)
    halo_recv(0, pads.at[0])

    def start_up(i, _):
        upstream[pl.ds(i * W, W), :] = cotangent[0, i].astype(F32)
        return 0

    lax.fori_loop(0, H, start_up, 0)

    def at(value, index, call):
        @pl.when(value == index)
        def _():
            call()

    blocks = J * (H // 8)
    spread_out = [(k, max(blocks * (2 * k + 1) // (2 * pieces), 1)) for k in range(pieces)]

    def first_conv(index):
        if not isinstance(index, int):
            for p, place in spread_out:
                at(index, place, lambda: weights_forward(0, 0, p))

    def first_norm():
        weights_got(0, 0, 0, 2)
        own_in[0].wait()

    def first_expand(s):
        def second(p):
            weights_second(0, 0, p)

        for p in range(pieces):
            if p:
                at(s, pieces + p, lambda: weights_got(0, 0, p, 2))
            at(s, 2 * pieces - 1 + p, lambda: second(p))
            at(s, 3 * pieces + p, lambda: weights_got(0, 0, p, 3))
            at(s, (2 * p + 1) * pieces, lambda: weights_forward(0, 1, p))

    def first_project(s):
        def one():
            for p in range(pieces):
                weights_got(0, 1, p, 2)

        def two():
            for p in range(pieces):
                weights_second(0, 1, p)

        def three():
            for p in range(pieces):
                weights_got(0, 1, p, 3)

        at(s, 0, lambda: own_out[0].wait())
        at(s, 1, one)
        at(s, 2, two)
        at(s, 3, three)

    def later(l):
        def in_conv(index):
            if isinstance(index, int):
                for p in range(pieces):
                    weights_second(l, 0, p)

        def in_norm():
            for p in range(pieces):
                weights_got(l, 0, p, 2)
                weights_got(l, 0, p, 3)
            own_in[l].wait()

        def in_expand(s):
            for p in range(pieces):
                at(s, NT // 2 + p, lambda: weights_second(l, 1, p))

        def in_project(s):
            def one():
                for p in range(pieces):
                    weights_got(l, 1, p, 2)
                own_out[l].wait()

            def three():
                for p in range(pieces):
                    weights_got(l, 1, p, 3)

            at(s, 0, one)
            at(s, 3, three)

        return dict(conv=in_conv, norm=in_norm, expand=in_expand, project=in_project)

    first = dict(
        conv=first_conv, norm=first_norm, expand=first_expand, project=first_project
    )
    for l in range(L):
        if l:
            for which in range(2):
                for p in range(pieces):
                    weights_forward(l, which, p)
            halo_recv(l, pads.at[l])
        forward(l, l == L - 1, later(l) if l else first)
        if l + 1 < L:
            halo_send(l + 1, pads.at[l + 1])

    clock = [0.0]
    due = []
    link = [0.0]

    def push(ready, chain, place, arg):
        due.append((ready, len(due), chain, place, arg))

    gchain = [
        (go_row, 4.0),
        (go_col, 4.0),
        (go_colg, 4.0),
        (go_rowg, 4.0),
        (go_coreg, 2.0),
        (go_out, 0.0),
    ]
    schain = [(small_second, 3.5), (small_third, 3.5), (small_fourth, 3.5), (small_end, 0)]

    def run_due(now):
        while due:
            best = min(due)
            if best[0] > now:
                return
            due.remove(best)
            ready, _, chain, place, arg = best
            chain[place][0](*arg)
            if place + 1 < len(chain):
                wait = chain[place][1]
                push(max(ready, clock[0]) + wait, chain, place + 1, arg)

    def spend(time):
        clock[0] += time
        run_due(clock[0])

    TILE, CONV, TAP = 1.0, 0.55, 0.75
    cut = 4
    for n, l in enumerate(reversed(range(L))):
        last = l == 0

        def hooks(name, index, l=l, last=last):
            if name == 'tile':
                start = clock[0]
                for t in range(NT):
                    clock[0] = start + (t + 1) * TILE
                    ready_now = [x for x in due if x[0] <= clock[0]]
                    if ready_now:
                        at(index, t, lambda: run_due(clock[0]))
                for t in range(NT):
                    begin = max(link[0], start + TILE * min(t + 3, NT))
                    link[0] = begin + 2.75
                    push(link[0] + 2.3, gchain, 0, (l, t))
            elif name == 'rest':
                spend(0.8)
            elif name == 'sent':
                spend(1.4)
                if last:
                    for k in range(1, L):
                        tap_sums(k, cut, 7, lambda q: spend(TAP))
                        small_start(k)
                        push(clock[0] + 3.5, schain, 0, (k,))
                    tap_sums(l, 0, 7, lambda q: spend(TAP))
                    small_start(l)
                    push(clock[0] + 3.5, schain, 0, (l,))
                else:
                    tap_sums(l, 0, cut, lambda q: spend(TAP))
            elif name == 'conv':
                start = clock[0]
                for k in range(blocks):
                    clock[0] = start + (k + 1) * CONV
                    if [x for x in due if x[0] <= clock[0]]:
                        at(index, k, lambda: run_due(clock[0]))

        backward(l, L + n, hooks, last)
        spend(0.8)
    while due:
        clock[0] = max(clock[0], min(due)[0])
        run_due(clock[0])
    for l in range(L):
        pltpu.sync_copy(small_out.at[l], out_small.at[l])

    def drain(t, _):
        for l in range(L):
            for copy in out_copies(l, t):
                copy.wait()
        return 0

    lax.fori_loop(0, NT, drain, 0)


def per_device(
    sizes,
    slides,
    cotangent,
    kernel,
    kernel_bias,
    norm_gain,
    norm_bias,
    weight_in,
    bias_in,
    weight_out,
    bias_out,
    layer_scale,
):
    R, C, DP = sizes["row"], sizes["col"], sizes["dp"]
    CD = C * DP
    L, DH, FF = weight_in.shape
    D = slides.shape[-1]
    H, W = slides.shape[1], slides.shape[2]
    N = H * W
    J = D // LANES
    T = DH
    NT = FF // T
    UN = DH // UNIT
    everyone = R * CD
    need = -(-(54 + FF // D) // 8) * J
    M = -(-need // everyone)
    row_units, count, bit, nb = 0, UN, 2, 0
    while bit < R:
        halve = count // 2 >= C
        count = count // 2 if halve else count
        row_units += count
        bit *= 2
        nb += 1
    per_col = count // C
    stages = 2 + nb + 2 * (C - 1) + nb + 1
    small_peers = max(R, CD) - 1
    vmem = pl.BlockSpec(memory_space=pltpu.VMEM)
    hbm = pl.BlockSpec(memory_space=pl.ANY)
    V = pltpu.VMEM
    DMA = pltpu.SemaphoreType.DMA
    turns = 2 * L
    out = pl.pallas_call(
        functools.partial(step_body, sizes),
        out_shape=(
            jax.ShapeDtypeStruct((1, H, W, D), BF16),
            jax.ShapeDtypeStruct((1, H, W, D), BF16),
            jax.ShapeDtypeStruct((L, UN, UNIT, FF), BF16),
            jax.ShapeDtypeStruct((L, UN, UNIT, FF), BF16),
            jax.ShapeDtypeStruct((L, R, CD, M, 8, LANES), F32),
        ),
        in_specs=[vmem] * 6 + [hbm, vmem, hbm, vmem, vmem],
        out_specs=(vmem, vmem, hbm, hbm, hbm),
        scratch_shapes=[
            V((L, J, H + 6, W + 2 * LEFT, LANES), F32),
            V((L, J, H + 6, W + 2 * LEFT, LANES), F32),
            V((L, J, 49, LANES), F32),
            V((J, H, W, LANES), F32),
            V((L, D, FF), BF16),
            V((L, NT, T, D), BF16),
            V((L, N, D), F32),
            V((L, N, 1), F32),
            V((L, N, D), BF16),
            V((L, D, N), BF16),
            V((L, NT, N, T), BF16),
            V((L, NT, N, T), BF16),
            V((L, N, D), F32),
            V((N, D), F32),
            V((N, D), BF16),
            V((D, N), BF16),
            V((N, D), F32),
            V((NT, 1, T), F32),
            V((J, 1, LANES), F32),
            V((L, NT, 2, DP, UN, UNIT, T), BF16),
            V((L, NT, DP, UN, UNIT, T), BF16),
            V((L, NT, UN, UNIT, T), BF16),
            V((L, NT, max(row_units, 1), UNIT, T), BF16),
            V((L, NT, max(C - 1, 1), per_col, UNIT, T), BF16),
            V((L, 2, NT, UN, UNIT, T), BF16),
            V((L, R, CD, M, 8, LANES), F32),
            V((L, max(R - 1, 1), CD, M, 8, LANES), F32),
            V((L, max(CD - 1, 1), M, 8, LANES), F32),
            V((L, R, CD, M, 8, LANES), F32),
            V((2, 3, W, D), BF16),
            V((2, 3, H, D), BF16),
            V((4, UNIT, D), BF16),
            V((turns, 2, 3, W, D), BF16),
            V((turns, 2, 3, H, D), BF16),
            V((turns, 4, UNIT, D), BF16),
            V((UNIT, D), F32),
            DMA((L, 2)),
            DMA((4, 4 * L)),
            DMA((4, 4 * L)),
            DMA((8,)),
            DMA((turns, 8)),
            DMA((NT, stages)),
            DMA((L, NT, stages)),
            DMA((4, small_peers)),
            DMA((L, 4, small_peers)),
            DMA((2, L, NT)),
        ],
        compiler_params=pltpu.CompilerParams(
            collective_id=0, has_side_effects=True, vmem_limit_bytes=67043328
        ),
        name="step",
    )(
        slides,
        cotangent,
        kernel.transpose(1, 2, 0, 3),
        kernel_bias,
        norm_gain,
        norm_bias,
        weight_in,
        bias_in,
        weight_out.reshape(L, NT, T, DH),
        bias_out,
        layer_scale,
    )
    return widen(*out, FF)


def widen_body(output, grad_slides, low_in, low_out, small, *outs):
    outs[0][...] = output[...]
    outs[1][...] = grad_slides[...]
    outs[2][...] = low_in[...].astype(F32)
    outs[3][0] = low_out[0].astype(F32).T
    taps, channel, bias = outs[4:]

    @pl.when(pl.program_id(0) == 0)
    def _():
        L, D = channel.shape[1], channel.shape[2]
        J = D // LANES
        for l in range(L):
            for line in range(54 + bias.shape[1] // D):
                for j in range(J):
                    unit = (line // 8) * J + j
                    value = small[l, unit, line % 8 : line % 8 + 1, :]
                    lane = j * LANES
                    if line < 49:
                        taps[
                            line // 7, line % 7, l : l + 1, lane : lane + LANES
                        ] = value
                    elif line < 54:
                        channel[line - 49, l : l + 1, lane : lane + LANES] = value
                    else:
                        lane += (line - 54) * D
                        bias[l : l + 1, lane : lane + LANES] = value


def widen(output, grad_slides, low_in, low_out, small, FF):
    _, H, W, D = output.shape
    L, DH = low_in.shape[0], low_in.shape[1] * low_in.shape[2]
    small = small.reshape(L, -1, 8, LANES)
    low_in = low_in.reshape(L, DH, FF)
    low_out = low_out.reshape(L, DH, FF)
    parts = 2
    steps = L * parts
    rows = -(-H // steps)
    maps = pl.BlockSpec((1, rows, W, D), lambda i: (0, i, 0, 0))
    wide = pl.BlockSpec((1, DH // parts, FF), lambda i: (i // parts, i % parts, 0))
    long = pl.BlockSpec((1, FF // parts, DH), lambda i: (i // parts, i % parts, 0))
    flat = pl.BlockSpec((1, DH, FF // parts), lambda i: (i // parts, 0, i % parts))

    def whole(shape):
        return pl.BlockSpec(shape, lambda i: (0,) * len(shape))

    shapes = (
        jax.ShapeDtypeStruct(output.shape, BF16),
        jax.ShapeDtypeStruct(output.shape, BF16),
        jax.ShapeDtypeStruct(low_in.shape, F32),
        jax.ShapeDtypeStruct((L, FF, DH), F32),
        jax.ShapeDtypeStruct((7, 7, L, D), F32),
        jax.ShapeDtypeStruct((5, L, D), F32),
        jax.ShapeDtypeStruct((L, FF), F32),
    )
    outs = pl.pallas_call(
        widen_body,
        grid=(steps,),
        out_shape=shapes,
        in_specs=[maps, maps, wide, flat, whole(small.shape)],
        out_specs=(maps, maps, wide, long) + tuple(whole(x.shape) for x in shapes[4:]),
        name="widen",
    )(output, grad_slides, low_in, low_out, small)
    return (
        *outs[:4],
        outs[4].transpose(2, 0, 1, 3),
        outs[5].transpose(1, 0, 2),
        outs[6],
    )


def solution(mesh):
    return jax.shard_map(
        functools.partial(per_device, dict(mesh.shape)),
        mesh=mesh,
        in_specs=(
            P("dp", "row", "col", None),
            P("dp", "row", "col", None),
            P(),
            P(),
            P(),
            P(),
            P(None, "dp", None),
            P(),
            P(None, None, "dp"),
            P(),
            P(),
        ),
        out_specs=(
            P("dp", "row", "col", None),
            P("dp", "row", "col", None),
            P(None, "dp", None),
            P(None, None, "dp"),
            P(),
            P(),
            P(),
        ),
        check_vma=False,
    )
```

```python
import functools

import jax
import jax.numpy as jnp
from jax import lax
from jax.experimental import pallas as pl
from jax.experimental.pallas import tpu as pltpu
from jax.sharding import PartitionSpec as P

COEF = 0.7978845608028654
CUBIC = 0.044715
EPSILON = 1e-06
LANES = 128
UNIT = 16
LEFT = 8
QUARTERS = 4
PAIR = 2
MESH = pl.DeviceIdType.MESH
F32 = jnp.float32
BF16 = jnp.bfloat16
STRAIGHT = ((-1, 0), (1, 0), (0, -1), (0, 1))
DIAGONAL = ((-1, -1), (-1, 1), (1, -1), (1, 1))
COLS = (((1,), (1,)), ((), ()))


def step_body(
    sizes,
    slides,
    cotangent,
    kernel,
    kernel_bias,
    norm_gain,
    norm_bias,
    weight_in,
    bias_in,
    weight_out,
    bias_out,
    layer_scale,
    output,
    grad_slides,
    out_in,
    out_out,
    out_small,
    pads,
    gpads,
    taps,
    mixed,
    win,
    wout,
    normed,
    rstd,
    normal,
    normal_t,
    act,
    slope,
    branch,
    upstream,
    gb_low,
    gb_t,
    gnorm,
    gbias,
    mixed_bias,
    grads,
    from_core,
    from_dp,
    from_row,
    from_col,
    early_row,
    early_col,
    early_dp,
    final,
    small,
    small_row,
    small_cd,
    small_out,
    row_send,
    col_send,
    cor_send,
    row_recv,
    col_recv,
    cor_recv,
    cor_wide,
    sem_local,
    sem_ws,
    sem_wr,
    sem_hs,
    sem_hr,
    sem_gs,
    sem_gr,
    sem_ss,
    sem_sr,
    sem_out,
):
    R, C, DP = sizes["row"], sizes["col"], sizes["dp"]
    CD = C * DP
    L, NT, _, T, D = wout.shape[0], wout.shape[1], 0, wout.shape[2], wout.shape[3]
    J = D // LANES
    H, W = slides.shape[1], slides.shape[2]
    N = H * W
    DH = D // DP
    UN = DH // UNIT
    row, col, dp = lax.axis_index("row"), lax.axis_index("col"), lax.axis_index("dp")
    cd = col * DP + dp
    core = row % 2

    def remote(src, dst, ssem, rsem, **where):
        return pltpu.make_async_remote_copy(
            src_ref=src,
            dst_ref=dst,
            send_sem=ssem,
            recv_sem=rsem,
            device_id=where,
            device_id_type=MESH,
        )

    def flip(index, bit):
        return index + bit - 2 * bit * ((index // bit) % 2)

    def there(dr, dc):
        ok = True
        if dr:
            ok = (row > 0) if dr < 0 else (row < R - 1)
        if dc:
            side = (col > 0) if dc < 0 else (col < C - 1)
            ok = side if ok is True else jnp.logical_and(ok, side)
        return ok

    def cd_peer(k):
        peer = (cd + k) % CD
        return peer, peer // DP, peer % DP

    barrier = pltpu.get_barrier_semaphore()
    for k in range(1, R):
        pl.semaphore_signal(
            barrier, inc=1, device_id={"row": (row + k) % R}, device_id_type=MESH
        )
    for k in range(1, CD):
        _, pc, pd = cd_peer(k)
        pl.semaphore_signal(
            barrier, inc=1, device_id={"col": pc, "dp": pd}, device_id_type=MESH
        )
    for dr, dc in DIAGONAL:

        @pl.when(there(dr, dc))
        def _():
            pl.semaphore_signal(
                barrier,
                inc=1,
                device_id={"row": row + dr, "col": col + dc},
                device_id_type=MESH,
            )

    own_in = [
        pltpu.make_async_copy(
            weight_in.at[l], win.at[l, pl.ds(dp * DH, DH), :], sem_local.at[l, 0]
        )
        for l in range(L)
    ]
    own_out = [
        pltpu.make_async_copy(
            weight_out.at[l],
            wout.at[l, :, :, pl.ds(dp * DH, DH)],
            sem_local.at[l, 1],
        )
        for l in range(L)
    ]
    for l in range(L):
        own_in[l].start()
        own_out[l].start()

    tall = H + 6
    zero_line = jnp.zeros((W + 2 * LEFT, LANES), F32)

    def clear(i, _):
        for j in range(J):
            for l in range(L):
                pads[l, j, i] = zero_line
                gpads[l, j, i] = zero_line
        return 0

    lax.fori_loop(0, tall, clear, 0)
    small[...] = jnp.zeros_like(small)
    for l in range(L):
        for p in range(7):
            for j in range(J):
                for q in range(7):
                    taps[l, j, 7 * p + q : 7 * p + q + 1, :] = kernel[
                        p, q, l : l + 1, j * LANES : (j + 1) * LANES
                    ]

    def fill(i, _):
        line = slides[0, i].astype(F32)
        for j in range(J):
            pads[0, j, i + 3, LEFT : LEFT + W, :] = line[:, j * LANES : (j + 1) * LANES]
        return 0

    lax.fori_loop(0, H, fill, 0)
    cor_wide[...] = jnp.zeros_like(cor_wide)

    def halo_copy(which, turn):
        if which < 4:
            dr, dc = STRAIGHT[which]
            if dr:
                src, dst = row_send.at[which], row_recv.at[turn, which]
            else:
                src, dst = col_send.at[which - 2], col_recv.at[turn, which - 2]
        else:
            dr, dc = DIAGONAL[which - 4]
            src, dst = cor_send.at[which - 4], cor_recv.at[turn, which - 4]
        where = {}
        if dr:
            where["row"] = row + dr
        if dc:
            where["col"] = col + dc
        return remote(src, dst, sem_hs.at[which], sem_hr.at[turn, which], **where)

    def lanes(j):
        return slice(j * LANES, (j + 1) * LANES)

    def halo_send(turn, src):
        for which, first in ((0, 3), (1, H)):
            for i in range(3):
                for j in range(J):
                    row_send[which, i, :, lanes(j)] = src[
                        j, first + i, LEFT : LEFT + W, :
                    ].astype(BF16)

            @pl.when(there(*STRAIGHT[which]))
            def _():
                halo_copy(which, turn).start()

        for which, first in ((2, LEFT), (3, LEFT + W - 3)):
            for i in range(3):
                for j in range(J):
                    col_send[which - 2, i, :, lanes(j)] = src[
                        j, 3 : 3 + H, first + i, :
                    ].astype(BF16)

            @pl.when(there(*STRAIGHT[which]))
            def _():
                halo_copy(which, turn).start()

        for k, (dr, dc) in enumerate(DIAGONAL):
            first, start = (3 if dr < 0 else H), (LEFT if dc < 0 else LEFT + W - 3)
            for i in range(3):
                for j in range(J):
                    cor_wide[3 * i : 3 * i + 3, lanes(j)] = src[
                        j, first + i, start : start + 3, :
                    ]
            cor_send[k] = cor_wide[...].astype(BF16)

            @pl.when(there(dr, dc))
            def _():
                halo_copy(4 + k, turn).start()

    def halo_recv(turn, dst):
        for which in (0, 1):
            first = H + 3 if which == 0 else 0
            dr, dc = STRAIGHT[which]

            @pl.when(there(-dr, -dc))
            def _():
                halo_copy(which, turn).wait_recv()
                for i in range(3):
                    line = row_recv[turn, which, i].astype(F32)
                    for j in range(J):
                        dst[j, first + i, LEFT : LEFT + W, :] = line[:, lanes(j)]

        for which in (2, 3):
            first = LEFT + W if which == 2 else LEFT - 3
            dr, dc = STRAIGHT[which]

            @pl.when(there(-dr, -dc))
            def _():
                halo_copy(which, turn).wait_recv()
                for i in range(3):
                    line = col_recv[turn, which - 2, i].astype(F32)
                    for j in range(J):
                        dst[j, 3 : 3 + H, first + i, :] = line[:, lanes(j)]

        for k, (dr, dc) in enumerate(DIAGONAL):
            first, start = (H + 3 if dr < 0 else 0), (LEFT + W if dc < 0 else LEFT - 3)

            @pl.when(there(-dr, -dc))
            def _():
                halo_copy(4 + k, turn).wait_recv()
                block = cor_recv[turn, k].astype(F32)
                for i in range(3):
                    for j in range(J):
                        dst[j, first + i, start : start + 3, :] = block[
                            3 * i : 3 * i + 3, lanes(j)
                        ]

        for which in range(8):
            dr, dc = (STRAIGHT + DIAGONAL)[which]

            @pl.when(there(dr, dc))
            def _():
                halo_copy(which, turn).wait_send()

    quarter = row % QUARTERS
    pieces = NT // QUARTERS

    def held(which, l, p, side, q):
        t = q * pieces + p
        if which == 0:
            cols = pl.ds(pl.multiple_of(t * T, T), T)
            return win.at[l, pl.ds(side * DH, DH), cols]
        return wout.at[l, t, :, pl.ds(side * DH, DH)]

    def own(which, l, p):
        t = quarter * pieces + p
        if which == 0:
            return weight_in.at[l, :, pl.ds(pl.multiple_of(t * T, T), T)]
        return weight_out.at[l, t]

    other = 1 - dp

    def w_x(l, which, p):
        k = (l * 2 + which) * pieces + p
        return remote(
            own(which, l, p),
            held(which, l, p, dp, quarter),
            sem_ws.at[0, k],
            sem_wr.at[0, k],
            dp=1 - dp,
        )

    def w_hop(l, which, p, stage):
        k = (l * 2 + which) * pieces + p
        bit = 2 if stage == 1 else 1
        q = flip(quarter, 2) if stage == 3 else quarter
        part = held(which, l, p, other, q)
        return remote(
            part, part, sem_ws.at[stage, k], sem_wr.at[stage, k], row=flip(row, bit)
        )

    def weights_x(l, which):
        for p in range(pieces):
            w_x(l, which, p).start()

    def weights_forward(l, which, p):
        w_x(l, which, p).wait()
        w_hop(l, which, p, 1).start()
        w_hop(l, which, p, 2).start()

    def weights_second(l, which, p):
        w_hop(l, which, p, 1).wait()
        w_hop(l, which, p, 3).start()

    def weights_got(l, which, p, stage):
        w_hop(l, which, p, stage).wait()

    def my_tile(s):
        q, p = s // pieces, s % pieces
        spot = flip(quarter, 1) * (q % 2) + quarter * (1 - q % 2)
        return ((spot + 2 * (q // 2)) % QUARTERS) * pieces + p

    def conv(src, l, mirrored, base, put, during=None):
        blocks = H // 8

        def one(index, _):
            j, start = index // blocks, (index % blocks) * 8
            totals = base(j, start)
            for q in range(7):
                for line in range(14):
                    window = src[
                        j, start + line, LEFT - 3 + q : LEFT - 3 + q + W, :
                    ]
                    for p in range(7):
                        i = line - p
                        if 0 <= i < 8:
                            k = 7 * p + q
                            k = 48 - k if mirrored else k
                            totals[i] = totals[i] + window * taps[l, j, k : k + 1, :]
            put(j, start, totals)
            if during is not None:
                during(index)
            return 0

        lax.fori_loop(0, J * blocks, one, 0)

    def tap_sums(l, first, end, during):
        for q in range(first, end):

            def lane_block(j, _):
                def block(index, totals):
                    start = index * 8
                    totals = list(totals)
                    for part in range(0, W, 8):
                        ups = [
                            gpads[
                                l, j, start + 3 + i, LEFT + part : LEFT + part + 8, :
                            ]
                            for i in range(8)
                        ]
                        for line in range(14):
                            first = LEFT - 3 + part + q
                            window = pads[l, j, start + line, first : first + 8, :]
                            for p in range(7):
                                i = line - p
                                if 0 <= i < 8:
                                    totals[p] = totals[p] + window * ups[i]
                    return tuple(totals)

                zero = jnp.zeros((8, LANES), F32)
                totals = lax.fori_loop(0, H // 8, block, (zero,) * 7)
                for p in range(7):
                    put_small(
                        l, 7 * p + q, j, jnp.sum(totals[p], axis=0, keepdims=True)
                    )
                return 0

            lax.fori_loop(0, J, lane_block, 0)
            during(q)

    M = small.shape[3]

    def put_small(l, line, j, value):
        unit = (line // 8) * J + j
        small[
            l, unit // (CD * M), (unit // M) % CD, unit % M, line % 8 : line % 8 + 1, :
        ] = value

    def put_row(l, line, value):
        for j in range(J):
            put_small(l, line, j, value[:, lanes(j)])

    def transpose(src, dst):
        for k in range(N // LANES):
            block = src[k * LANES : (k + 1) * LANES, :].astype(F32)
            dst[:, lanes(k)] = block.T.astype(BF16)

    def forward(l, last, hooks):
        bias_line = kernel_bias[l : l + 1, :]
        for j in range(J):
            mixed_bias[j] = bias_line[:, lanes(j)]

        def base(j, start):
            del start
            bias = mixed_bias[j]
            return [jnp.broadcast_to(bias, (W, LANES)) for _ in range(8)]

        def put(j, start, totals):
            for i in range(8):
                mixed[j, start + i] = totals[i]

        conv(pads.at[l], l, False, base, put, hooks["conv"])
        hooks["conv"](-1)
        gain, shift = norm_gain[l : l + 1, :], norm_bias[l : l + 1, :]

        def norm(i, _):
            lines = pl.ds(i * W, W)
            value = jnp.concatenate([mixed[j, i] for j in range(J)], axis=1)
            center = value - jnp.mean(value, -1, keepdims=True)
            scale = lax.rsqrt(jnp.mean(center * center, -1, keepdims=True) + EPSILON)
            out = center * scale
            normed[l, lines, :] = out
            rstd[l, lines, :] = scale
            normal[lines, :] = (out * gain + shift).astype(BF16)
            return 0

        lax.fori_loop(0, H, norm, 0, unroll=4)
        hooks["norm"]()
        transpose(normal, normal_t.at[l])

        group = hooks["group"]

        def expand(s, _):
            hooks["expand"](s)
            for k in range(group):
                t = my_tile(s * group + k)
                cols = pl.ds(pl.multiple_of(t * T, T), T)
                hidden = jnp.dot(normal[...], win[l, :, cols], preferred_element_type=F32)
                hidden = hidden + bias_in[l : l + 1, cols]
                square = hidden * hidden
                tangent = jnp.tanh(hidden * (COEF + (COEF * CUBIC) * square))
                both = 1.0 + tangent
                half = 0.5 * hidden
                act[l, t] = (half * both).astype(BF16)
                steep = half * (COEF + (3.0 * COEF * CUBIC) * square)
                slope[l, t] = (both * (0.5 + (1.0 - tangent) * steep)).astype(BF16)
            return 0

        lax.fori_loop(0, NT // group, expand, 0)
        branch[l] = jnp.broadcast_to(bias_out[l : l + 1, :], (N, D))

        def project(s, _):
            hooks["project"](s)
            total = branch[l]
            for p in range(pieces):
                t = my_tile(s * pieces + p)
                total = total + jnp.dot(
                    act[l, t], wout[l, t], preferred_element_type=F32
                )
            branch[l] = total
            return 0

        lax.fori_loop(0, QUARTERS, project, 0)
        scales = layer_scale[l : l + 1, :]

        def finish(i, _):
            part = scales * branch[l, pl.ds(i * W, W), :]
            for j in range(J):
                old = pads[l, j, i + 3, LEFT : LEFT + W, :]
                new = (old + part[:, lanes(j)]).astype(BF16)
                if last:
                    output[0, i, :, lanes(j)] = new
                else:
                    pads[l + 1, j, i + 3, LEFT : LEFT + W, :] = new.astype(F32)
            return 0

        lax.fori_loop(0, H, finish, 0)

    bits = []
    bit = 2
    while bit < R:
        bits.append(bit)
        bit *= 2
    levels = []
    count = UN
    for b in bits:
        halve = count // 2 >= C
        levels.append((b, count, halve))
        count = count // 2 if halve else count
    left_units = count
    per_col = left_units // C
    nb = len(bits)
    S_CORE, S_DP, S_ROW, S_COL = 0, 1, 2, 2 + nb
    S_COLG = S_COL + C - 1
    S_ROWG = S_COLG + C - 1
    S_COREG = S_ROWG + nb

    def unit_base(level):
        start = 0
        for b, n, halve in levels[:level]:
            if halve:
                start = start + ((row // b) % 2) * (n // 2)
        return start

    def g_core(l, t):
        return remote(
            grads.at[l, t, 1 - core],
            from_core.at[l, t],
            sem_gs.at[t, S_CORE],
            sem_gr.at[l, t, S_CORE],
            row=flip(row, 1),
        )

    def g_dp(l, t):
        return remote(
            grads.at[l, t, core, 1 - dp],
            from_dp.at[l, t],
            sem_gs.at[t, S_DP],
            sem_gr.at[l, t, S_DP],
            dp=1 - dp,
        )

    row_slot = []
    at = 0
    for b, n, halve in levels:
        row_slot.append(at)
        at += n // 2 if halve else n

    def g_row(l, t, level):
        b, n, halve = levels[level]
        mine = (row // b) % 2
        start = unit_base(level)
        m = n
        if halve:
            m = n // 2
            start = start + (1 - mine) * m
        return remote(
            grads.at[l, t, core, dp, pl.ds(start, m)],
            from_row.at[l, t, pl.ds(row_slot[level], m)],
            sem_gs.at[t, S_ROW + level],
            sem_gr.at[l, t, S_ROW + level],
            row=flip(row, b),
        )

    def g_row_add(l, t, level):
        b, n, halve = levels[level]
        start = unit_base(level + 1)
        m = n // 2 if halve else n
        mine = grads.at[l, t, core, dp, pl.ds(start, m)]
        mine[...] = mine[...] + from_row[l, t, pl.ds(row_slot[level], m)]

    col_base = unit_base(nb)

    def g_col(l, t, k):
        peer = (col + k) % C
        return remote(
            grads.at[l, t, core, dp, pl.ds(col_base + peer * per_col, per_col)],
            from_col.at[l, t, k - 1],
            sem_gs.at[t, S_COL + k - 1],
            sem_gr.at[l, t, S_COL + k - 1],
            col=peer,
        )

    def g_colg(l, t, k):
        peer = (col + k) % C
        part = final.at[l, core, t, pl.ds(col_base + col * per_col, per_col)]
        return remote(
            part,
            part,
            sem_gs.at[t, S_COLG + k - 1],
            sem_gr.at[l, t, S_COLG + k - 1],
            col=peer,
        )

    def g_rowg(l, t, level):
        b, n, halve = levels[level]
        part = final.at[l, core, t, pl.ds(unit_base(level + 1), n // 2)]
        return remote(
            part,
            part,
            sem_gs.at[t, S_ROWG + level],
            sem_gr.at[l, t, S_ROWG + level],
            row=flip(row, b),
        )

    def g_coreg(l, t):
        part = final.at[l, core, t]
        return remote(
            part,
            part,
            sem_gs.at[t, S_COREG],
            sem_gr.at[l, t, S_COREG],
            row=flip(row, 1),
        )

    def go_dp(l, t):
        g_core(l, t).wait()
        mine = grads.at[l, t, core]
        mine[...] = mine[...] + from_core[l, t]
        g_dp(l, t).start()

    def go_row(l, t):
        g_dp(l, t).wait()
        mine = grads.at[l, t, core, dp]
        mine[...] = mine[...] + from_dp[l, t]
        for level in range(nb):
            if level:
                g_row(l, t, level - 1).wait()
                g_row_add(l, t, level - 1)
            g_row(l, t, level).start()

    def go_col(l, t):
        if nb:
            g_row(l, t, nb - 1).wait()
            g_row_add(l, t, nb - 1)
        for k in range(1, C):
            g_col(l, t, k).start()

    def go_colg(l, t):
        for k in range(1, C):
            g_col(l, t, k).wait()
        place = pl.ds(col_base + col * per_col, per_col)
        total = grads[l, t, core, dp, place].astype(F32)
        for k in range(1, C):
            total = total + from_col[l, t, k - 1].astype(F32)
        final[l, core, t, place] = total.astype(BF16)
        for k in range(1, C):
            g_colg(l, t, k).start()

    halved = [k for k in range(nb) if levels[k][2]][::-1]

    def go_rowg(l, t):
        for k in range(1, C):
            g_colg(l, t, k).wait()
        for n, level in enumerate(halved):
            if n:
                g_rowg(l, t, halved[n - 1]).wait()
            g_rowg(l, t, level).start()

    def go_coreg(l, t):
        if halved:
            g_rowg(l, t, halved[-1]).wait()
        g_coreg(l, t).start()

    def h_row(l, t, level):
        b, n, halve = levels[level]
        start, m = unit_base(level), n
        if halve:
            m = n // 2
            start = start + (1 - (row // b) % 2) * m
        return remote(
            grads.at[l, t, core, :, pl.ds(start, m)],
            early_row.at[t, :, pl.ds(row_slot[level], m)],
            sem_gs.at[t, S_ROW + level],
            sem_gr.at[l, t, S_ROW + level],
            row=flip(row, b),
        )

    def h_row_add(l, t, level):
        _, n, halve = levels[level]
        m = n // 2 if halve else n
        mine = grads.at[l, t, core, :, pl.ds(unit_base(level + 1), m)]
        mine[...] = mine[...] + early_row[t, :, pl.ds(row_slot[level], m)]

    def h_col(l, t, k):
        peer = (col + k) % C
        return remote(
            grads.at[l, t, core, :, pl.ds(col_base + peer * per_col, per_col)],
            early_col.at[t, k - 1],
            sem_gs.at[t, S_COL + k - 1],
            sem_gr.at[l, t, S_COL + k - 1],
            col=peer,
        )

    my_units = pl.ds(col_base + col * per_col, per_col)

    def h_dp(l, t):
        return remote(
            grads.at[l, t, core, 1 - dp, my_units],
            early_dp.at[t],
            sem_gs.at[t, S_DP],
            sem_gr.at[l, t, S_DP],
            dp=1 - dp,
        )

    def early_start(l, t):
        g_core(l, t).wait()
        mine = grads.at[l, t, core]
        mine[...] = mine[...] + from_core[l, t]
        for level in range(nb):
            if level:
                h_row(l, t, level - 1).wait()
                h_row_add(l, t, level - 1)
            h_row(l, t, level).start()

    def early_col_go(l, t):
        if nb:
            h_row(l, t, nb - 1).wait()
            h_row_add(l, t, nb - 1)
        for k in range(1, C):
            h_col(l, t, k).start()

    def early_dp_go(l, t):
        for k in range(1, C):
            h_col(l, t, k).wait()
        total = grads[l, t, core, :, my_units].astype(F32)
        for k in range(1, C):
            total = total + early_col[t, k - 1].astype(F32)
        grads[l, t, core, :, my_units] = total.astype(BF16)
        h_dp(l, t).start()

    def early_colg(l, t):
        h_dp(l, t).wait()
        final[l, core, t, my_units] = grads[l, t, core, dp, my_units] + early_dp[t]
        for k in range(1, C):
            g_colg(l, t, k).start()

    def out_copies(l, t):
        cols = pl.ds(pl.multiple_of(t * T, T), T)
        return (
            pltpu.make_async_copy(
                final.at[l, 0, t], out_in.at[l, :, :, cols], sem_out.at[0, l, t]
            ),
            pltpu.make_async_copy(
                final.at[l, 1, t], out_out.at[l, :, :, cols], sem_out.at[1, l, t]
            ),
        )

    def go_out(l, t):
        g_coreg(l, t).wait()
        for copy in out_copies(l, t):
            copy.start()

    chain = (go_row, go_col, go_colg, go_rowg, go_coreg, go_out)

    def s_copy(l, stage, k):
        if stage in (0, 3):
            peer = (row + k) % R
            where = {"row": peer}
        else:
            peer, pc, pd = cd_peer(k)
            where = {"col": pc, "dp": pd}
        if stage == 0:
            src, dst = small.at[l, peer], small_row.at[l, k - 1]
        elif stage == 1:
            src, dst = small.at[l, row, peer], small_cd.at[l, k - 1]
        elif stage == 2:
            src = dst = small_out.at[l, row, cd]
        else:
            src = dst = small_out.at[l, row]
        return remote(
            src, dst, sem_ss.at[stage, k - 1], sem_sr.at[l, stage, k - 1], **where
        )

    def small_start(l):
        for k in range(1, R):
            s_copy(l, 0, k).start()

    def small_second(l):
        for k in range(1, R):
            s_copy(l, 0, k).wait()
        total = small[l, row]
        for k in range(1, R):
            total = total + small_row[l, k - 1]
        small[l, row] = total
        for k in range(1, CD):
            s_copy(l, 1, k).start()

    def small_third(l):
        for k in range(1, CD):
            s_copy(l, 1, k).wait()
        total = small[l, row, cd]
        for k in range(1, CD):
            total = total + small_cd[l, k - 1]
        small_out[l, row, cd] = total
        for k in range(1, CD):
            s_copy(l, 2, k).start()

    def small_fourth(l):
        for k in range(1, CD):
            s_copy(l, 2, k).wait()
        for k in range(1, R):
            s_copy(l, 3, k).start()

    def small_end(l):
        for k in range(1, R):
            s_copy(l, 3, k).wait()

    def backward(l, turn, hooks, last):
        gpad = gpads.at[l]
        scales = layer_scale[l : l + 1, :]
        empty = jnp.zeros((8, D), F32)

        def fold(value):
            total = value[0:8]
            for k in range(8, value.shape[0], 8):
                total = total + value[k : k + 8]
            return total

        def before(i, sums):
            lines = pl.ds(i * W, W)
            up = upstream[lines, :]
            gb = up * scales
            gb_low[lines, :] = gb.astype(BF16)
            return (sums[0] + fold(up * branch[l, lines, :]), sums[1] + fold(gb))

        sums = lax.fori_loop(0, H, before, (empty,) * 2)
        put_row(l, 53, jnp.sum(sums[0], 0, keepdims=True))
        put_row(l, 52, jnp.sum(sums[1], 0, keepdims=True))
        gnorm[...] = jnp.zeros_like(gnorm)
        transpose(gb_low, gb_t)

        def pair(i, _):
            first_late = 2
            if l == L - 1:
                first_late = 3

                @pl.when(i == 2)
                def _():
                    for k in range(PAIR):
                        early_start(l, k)

            @pl.when(i >= first_late)
            def _():
                for k in range(PAIR):
                    go_dp(l, (i - 2) * PAIR + k)

            hooks('tile', i)
            gb, gb_turned = gb_low[...], gb_t[...]
            lows = []
            for k in range(PAIR):
                t = i * PAIR + k
                ga = lax.dot_general(gb, wout[l, t], COLS, preferred_element_type=F32)
                gh = ga * slope[l, t].astype(F32)
                gbias[t] = jnp.sum(gh, 0, keepdims=True)
                lows.append(gh.astype(BF16))
            for k in range(PAIR):
                t = i * PAIR + k
                g_out = jnp.dot(gb_turned, act[l, t], preferred_element_type=F32)
                grads[l, t, 1] = g_out.astype(BF16).reshape(DP, UN, UNIT, T)
            total = gnorm[...]
            for k in range(PAIR):
                t = i * PAIR + k
                g_in = jnp.dot(normal_t[l], lows[k], preferred_element_type=F32)
                grads[l, t, 0] = g_in.astype(BF16).reshape(DP, UN, UNIT, T)
                cols = pl.ds(pl.multiple_of(t * T, T), T)
                total = total + lax.dot_general(
                    lows[k], win[l, :, cols], COLS, preferred_element_type=F32
                )
            gnorm[...] = total
            for k in range(PAIR):
                g_core(l, i * PAIR + k).start()
            return 0

        lax.fori_loop(0, NT // PAIR, pair, 0)
        for t in range(NT - 2 * PAIR, NT - PAIR):
            go_dp(l, t)
        hooks('rest', -1)
        per_line = D // T
        for t in range(NT):
            for half in range(T // LANES):
                j = (t % per_line) * (T // LANES) + half
                put_small(l, 54 + t // per_line, j, gbias[t, :, lanes(half)])
        gain = norm_gain[l : l + 1, :]

        def after(i, sums):
            lines = pl.ds(i * W, W)
            gn, unit = gnorm[lines, :], normed[l, lines, :]
            both = gn * unit
            gs = gn * gain
            first = jnp.mean(gs, -1, keepdims=True)
            second = jnp.mean(gs * unit, -1, keepdims=True)
            gm = rstd[l, lines, :] * (gs - first - unit * second)
            for j in range(J):
                gpad[j, i + 3, LEFT : LEFT + W, :] = gm[:, lanes(j)]
            return (sums[0] + fold(gm), sums[1] + fold(both), sums[2] + fold(gn))

        sums = lax.fori_loop(0, H, after, (empty,) * 3, unroll=2)
        for k in range(3):
            put_row(l, 49 + k, jnp.sum(sums[k], 0, keepdims=True))
        halo_send(turn, gpad)
        for t in range(NT - PAIR, NT):
            go_dp(l, t)
        hooks('sent', -1)
        halo_recv(turn, gpad)

        def base(j, start):
            return [up_block[j, start + i] for i in range(8)]

        up_block = mixed

        def spread(i, _):
            for j in range(J):
                mixed[j, i] = upstream[pl.ds(i * W, W), lanes(j)]
            return 0

        lax.fori_loop(0, H, spread, 0)

        def put(j, start, totals):
            for i in range(8):
                mixed[j, start + i] = totals[i]

        conv(gpad, l, True, base, put, lambda k: hooks('conv', k))

        def gather(i, _):
            for j in range(J):
                if last:
                    grad_slides[0, i, :, lanes(j)] = mixed[j, i].astype(BF16)
                else:
                    upstream[pl.ds(i * W, W), lanes(j)] = mixed[j, i]
            return 0

        lax.fori_loop(0, H, gather, 0)

    diagonals = jnp.where(row > 0, 1, 0) + jnp.where(row < R - 1, 1, 0)
    diagonals = diagonals * (
        jnp.where(col > 0, 1, 0) + jnp.where(col < C - 1, 1, 0)
    )
    pl.semaphore_wait(barrier, R - 1 + CD - 1 + diagonals)
    halo_send(0, pads.at[0])
    for l in range(L):
        for which in range(2):
            weights_x(l, which)
    halo_recv(0, pads.at[0])

    def start_up(i, _):
        upstream[pl.ds(i * W, W), :] = cotangent[0, i].astype(F32)
        return 0

    lax.fori_loop(0, H, start_up, 0)

    def at(value, index, call):
        @pl.when(value == index)
        def _():
            call()

    blocks = J * (H // 8)
    spread_out = [(k, max(blocks * (2 * k + 1) // (2 * pieces), 1)) for k in range(pieces)]

    def first_conv(index):
        if not isinstance(index, int):
            for p, place in spread_out:
                at(index, place, lambda: weights_forward(0, 0, p))

    def first_norm():
        weights_got(0, 0, 0, 2)
        own_in[0].wait()

    def first_expand(s):
        def second(p):
            weights_second(0, 0, p)

        for p in range(pieces):
            if p:
                at(s, pieces + p, lambda: weights_got(0, 0, p, 2))
            at(s, 2 * pieces - 1 + p, lambda: second(p))
            at(s, 3 * pieces + p, lambda: weights_got(0, 0, p, 3))
            at(s, (2 * p + 1) * pieces, lambda: weights_forward(0, 1, p))

    def first_project(s):
        def one():
            for p in range(pieces):
                weights_got(0, 1, p, 2)

        def two():
            for p in range(pieces):
                weights_second(0, 1, p)

        def three():
            for p in range(pieces):
                weights_got(0, 1, p, 3)

        at(s, 0, lambda: own_out[0].wait())
        at(s, 1, one)
        at(s, 2, two)
        at(s, 3, three)
        if L > 1:
            for p in range(pieces):
                at(s, min(1 + p, QUARTERS - 1), lambda: weights_forward(1, 0, p))

    def later(l):
        def in_conv(index):
            if isinstance(index, int):
                weights_second(l, 0, pieces - 1)
                return
            for p in range(pieces):
                at(index, min(1 + 3 * p, blocks - 1), lambda: weights_forward(l, 1, p))
                if p + 1 < pieces:
                    at(index, blocks - 2, lambda: weights_second(l, 0, p))

        def in_norm():
            for p in range(pieces):
                weights_got(l, 0, p, 2)
                weights_got(l, 0, p, 3)
            own_in[l].wait()

        def in_expand(s):
            for p in range(pieces):
                at(s, min(1 + 2 * p, QUARTERS - 1), lambda: weights_second(l, 1, p))

        def in_project(s):
            def one():
                for p in range(pieces):
                    weights_got(l, 1, p, 2)
                own_out[l].wait()

            def three():
                for p in range(pieces):
                    weights_got(l, 1, p, 3)

            at(s, 0, one)
            at(s, 3, three)

        return dict(
            conv=in_conv,
            norm=in_norm,
            expand=in_expand,
            project=in_project,
            group=pieces,
        )

    first = dict(
        conv=first_conv,
        norm=first_norm,
        expand=first_expand,
        project=first_project,
        group=1,
    )
    for l in range(L):
        if l:
            for p in range(pieces if l > 1 else 0):
                weights_forward(l, 0, p)
            halo_recv(l, pads.at[l])
        forward(l, l == L - 1, later(l) if l else first)
        if l + 1 < L:
            halo_send(l + 1, pads.at[l + 1])

    clock = [0.0]
    due = []
    link = [0.0]
    serial = [0]
    cross = [0.0]

    def push(ready, chain, place, arg):
        serial[0] += 1
        due.append((ready, serial[0], chain, place, arg))

    gchain = [
        (go_row, 4.0),
        (go_col, 4.8),
        (go_colg, 4.8),
        (go_rowg, 4.0),
        (go_coreg, 9.0),
        (go_out, 0.0),
    ]
    echain = [(early_col_go, 4.8), (early_dp_go, 5.4), (early_colg, 3.5)] + gchain[3:]
    echain[2] = (early_colg, 3.5)
    schain = [(small_second, 5.0), (small_third, 5.0), (small_fourth, 6.0), (small_end, 0)]

    def run_due(now):
        while due:
            best = min(due)
            if best[0] > now:
                return
            due.remove(best)
            ready, _, chain, place, arg = best
            chain[place][0](*arg)
            if place + 1 < len(chain):
                wait = chain[place][1]
                soon = max(ready, clock[0]) + wait
                if chain is echain and place == 1:
                    link[0] = max(link[0], clock[0]) + 0.35
                    soon = link[0] + 3.0
                if chain is schain and place == 0:
                    soon = max(soon, link[0] + 4.0)
                push(soon, chain, place + 1, arg)

    def spend(time):
        clock[0] += time
        run_due(clock[0])

    TILE, CONV, TAP = 1.4, 0.57, 0.75
    cut = 4
    for n, l in enumerate(reversed(range(L))):
        last = l == 0

        def hooks(name, index, l=l, last=last):
            if name == 'tile':
                start = clock[0]
                for t in range(NT // PAIR):
                    clock[0] = start + t * TILE
                    ready_now = [x for x in due if x[0] <= clock[0]]
                    if ready_now:
                        at(index, t, lambda: run_due(clock[0]))
                clock[0] = start + TILE * NT // PAIR
                for t in range(NT):
                    begin = start + TILE * min(t // PAIR + 2, NT // PAIR)
                    if l == L - 1 and t < PAIR:
                        cross[0] = max(cross[0], begin) + 2.75
                        push(cross[0] + 2.3, echain, 0, (l, t))
                        continue
                    begin = max(link[0], begin)
                    link[0] = begin + 2.75
                    push(link[0] + 2.3, gchain, 0, (l, t))
            elif name == 'rest':
                spend(0.8)
            elif name == 'sent':
                spend(1.4)
                if last:
                    for k in range(1, L):
                        tap_sums(k, cut, 7, lambda q: spend(TAP))
                        small_start(k)
                        push(clock[0] + 5.0, schain, 0, (k,))
                    tap_sums(l, 0, 7, lambda q: spend(TAP))
                    small_start(l)
                    push(clock[0] + 5.0, schain, 0, (l,))
                else:
                    tap_sums(l, 0, cut, lambda q: spend(TAP))
            elif name == 'conv':
                start = clock[0]
                for k in range(blocks):
                    clock[0] = start + (k + 1) * CONV
                    if [x for x in due if x[0] <= clock[0]]:
                        at(index, k, lambda: run_due(clock[0]))

        backward(l, L + n, hooks, last)
        spend(0.8)
    while due:
        clock[0] = max(clock[0], min(due)[0])
        run_due(clock[0])
    for l in range(L):
        pltpu.sync_copy(small_out.at[l], out_small.at[l])

    def drain(t, _):
        for l in range(L):
            for copy in out_copies(l, t):
                copy.wait()
        return 0

    lax.fori_loop(0, NT, drain, 0)


def per_device(
    sizes,
    slides,
    cotangent,
    kernel,
    kernel_bias,
    norm_gain,
    norm_bias,
    weight_in,
    bias_in,
    weight_out,
    bias_out,
    layer_scale,
):
    R, C, DP = sizes["row"], sizes["col"], sizes["dp"]
    CD = C * DP
    L, DH, FF = weight_in.shape
    D = slides.shape[-1]
    H, W = slides.shape[1], slides.shape[2]
    N = H * W
    J = D // LANES
    T = DH
    NT = FF // T
    UN = DH // UNIT
    everyone = R * CD
    need = -(-(54 + FF // D) // 8) * J
    M = -(-need // everyone)
    row_units, count, bit, nb = 0, UN, 2, 0
    while bit < R:
        halve = count // 2 >= C
        count = count // 2 if halve else count
        row_units += count
        bit *= 2
        nb += 1
    per_col = count // C
    early = PAIR
    stages = 2 + nb + 2 * (C - 1) + nb + 1
    small_peers = max(R, CD) - 1
    vmem = pl.BlockSpec(memory_space=pltpu.VMEM)
    hbm = pl.BlockSpec(memory_space=pl.ANY)
    V = pltpu.VMEM
    DMA = pltpu.SemaphoreType.DMA
    turns = 2 * L
    out = pl.pallas_call(
        functools.partial(step_body, sizes),
        out_shape=(
            jax.ShapeDtypeStruct((1, H, W, D), BF16),
            jax.ShapeDtypeStruct((1, H, W, D), BF16),
            jax.ShapeDtypeStruct((L, UN, UNIT, FF), BF16),
            jax.ShapeDtypeStruct((L, UN, UNIT, FF), BF16),
            jax.ShapeDtypeStruct((L, R, CD, M, 8, LANES), F32),
        ),
        in_specs=[vmem] * 6 + [hbm, vmem, hbm, vmem, vmem],
        out_specs=(vmem, vmem, hbm, hbm, hbm),
        scratch_shapes=[
            V((L, J, H + 6, W + 2 * LEFT, LANES), F32),
            V((L, J, H + 6, W + 2 * LEFT, LANES), F32),
            V((L, J, 49, LANES), F32),
            V((J, H, W, LANES), F32),
            V((L, D, FF), BF16),
            V((L, NT, T, D), BF16),
            V((L, N, D), F32),
            V((L, N, 1), F32),
            V((N, D), BF16),
            V((L, D, N), BF16),
            V((L, NT, N, T), BF16),
            V((L, NT, N, T), BF16),
            V((L, N, D), F32),
            V((N, D), F32),
            V((N, D), BF16),
            V((D, N), BF16),
            V((N, D), F32),
            V((NT, 1, T), F32),
            V((J, 1, LANES), F32),
            V((L, NT, 2, DP, UN, UNIT, T), BF16),
            V((L, NT, DP, UN, UNIT, T), BF16),
            V((L, NT, UN, UNIT, T), BF16),
            V((L, NT, max(row_units, 1), UNIT, T), BF16),
            V((L, NT, max(C - 1, 1), per_col, UNIT, T), BF16),
            V((early, DP, max(row_units, 1), UNIT, T), BF16),
            V((early, max(C - 1, 1), DP, per_col, UNIT, T), BF16),
            V((early, per_col, UNIT, T), BF16),
            V((L, 2, NT, UN, UNIT, T), BF16),
            V((L, R, CD, M, 8, LANES), F32),
            V((L, max(R - 1, 1), CD, M, 8, LANES), F32),
            V((L, max(CD - 1, 1), M, 8, LANES), F32),
            V((L, R, CD, M, 8, LANES), F32),
            V((2, 3, W, D), BF16),
            V((2, 3, H, D), BF16),
            V((4, UNIT, D), BF16),
            V((turns, 2, 3, W, D), BF16),
            V((turns, 2, 3, H, D), BF16),
            V((turns, 4, UNIT, D), BF16),
            V((UNIT, D), F32),
            DMA((L, 2)),
            DMA((4, 4 * L)),
            DMA((4, 4 * L)),
            DMA((8,)),
            DMA((turns, 8)),
            DMA((NT, stages)),
            DMA((L, NT, stages)),
            DMA((4, small_peers)),
            DMA((L, 4, small_peers)),
            DMA((2, L, NT)),
        ],
        compiler_params=pltpu.CompilerParams(
            collective_id=0, has_side_effects=True, vmem_limit_bytes=67043328
        ),
        name="step",
    )(
        slides,
        cotangent,
        kernel.transpose(1, 2, 0, 3),
        kernel_bias,
        norm_gain,
        norm_bias,
        weight_in,
        bias_in,
        weight_out.reshape(L, NT, T, DH),
        bias_out,
        layer_scale,
    )
    return widen(*out, FF)


def widen_body(output, grad_slides, low_in, low_out, small, *outs):
    outs[0][...] = output[...]
    outs[1][...] = grad_slides[...]
    outs[2][...] = low_in[...].astype(F32)
    outs[3][0] = low_out[0].astype(F32).T
    taps, channel, bias = outs[4:]

    @pl.when(pl.program_id(0) == 0)
    def _():
        L, D = channel.shape[1], channel.shape[2]
        J = D // LANES
        for l in range(L):
            for line in range(54 + bias.shape[1] // D):
                for j in range(J):
                    unit = (line // 8) * J + j
                    value = small[l, unit, line % 8 : line % 8 + 1, :]
                    lane = j * LANES
                    if line < 49:
                        taps[
                            line // 7, line % 7, l : l + 1, lane : lane + LANES
                        ] = value
                    elif line < 54:
                        channel[line - 49, l : l + 1, lane : lane + LANES] = value
                    else:
                        lane += (line - 54) * D
                        bias[l : l + 1, lane : lane + LANES] = value


def widen(output, grad_slides, low_in, low_out, small, FF):
    _, H, W, D = output.shape
    L, DH = low_in.shape[0], low_in.shape[1] * low_in.shape[2]
    small = small.reshape(L, -1, 8, LANES)
    low_in = low_in.reshape(L, DH, FF)
    low_out = low_out.reshape(L, DH, FF)
    parts = 2
    steps = L * parts
    rows = -(-H // steps)
    maps = pl.BlockSpec((1, rows, W, D), lambda i: (0, i, 0, 0))
    wide = pl.BlockSpec((1, DH // parts, FF), lambda i: (i // parts, i % parts, 0))
    long = pl.BlockSpec((1, FF // parts, DH), lambda i: (i // parts, i % parts, 0))
    flat = pl.BlockSpec((1, DH, FF // parts), lambda i: (i // parts, 0, i % parts))

    def whole(shape):
        return pl.BlockSpec(shape, lambda i: (0,) * len(shape))

    shapes = (
        jax.ShapeDtypeStruct(output.shape, BF16),
        jax.ShapeDtypeStruct(output.shape, BF16),
        jax.ShapeDtypeStruct(low_in.shape, F32),
        jax.ShapeDtypeStruct((L, FF, DH), F32),
        jax.ShapeDtypeStruct((7, 7, L, D), F32),
        jax.ShapeDtypeStruct((5, L, D), F32),
        jax.ShapeDtypeStruct((L, FF), F32),
    )
    outs = pl.pallas_call(
        widen_body,
        grid=(steps,),
        out_shape=shapes,
        in_specs=[maps, maps, wide, flat, whole(small.shape)],
        out_specs=(maps, maps, wide, long) + tuple(whole(x.shape) for x in shapes[4:]),
        name="widen",
    )(output, grad_slides, low_in, low_out, small)
    return (
        *outs[:4],
        outs[4].transpose(2, 0, 1, 3),
        outs[5].transpose(1, 0, 2),
        outs[6],
    )


def solution(mesh):
    return jax.shard_map(
        functools.partial(per_device, dict(mesh.shape)),
        mesh=mesh,
        in_specs=(
            P("dp", "row", "col", None),
            P("dp", "row", "col", None),
            P(),
            P(),
            P(),
            P(),
            P(None, "dp", None),
            P(),
            P(None, None, "dp"),
            P(),
            P(),
        ),
        out_specs=(
            P("dp", "row", "col", None),
            P("dp", "row", "col", None),
            P(None, "dp", None),
            P(None, None, "dp"),
            P(),
            P(),
            P(),
        ),
        check_vma=False,
    )
```

```python
import functools

import jax
import jax.numpy as jnp
from jax import lax
from jax.experimental import pallas as pl
from jax.experimental.pallas import tpu as pltpu
from jax.sharding import PartitionSpec as P

COEF = 0.7978845608028654
CUBIC = 0.044715
EPSILON = 1e-06
LANES = 128
UNIT = 16
LEFT = 8
QUARTERS = 4
PAIR = 2
MESH = pl.DeviceIdType.MESH
F32 = jnp.float32
BF16 = jnp.bfloat16
STRAIGHT = ((-1, 0), (1, 0), (0, -1), (0, 1))
DIAGONAL = ((-1, -1), (-1, 1), (1, -1), (1, 1))
COLS = (((1,), (1,)), ((), ()))


def step_body(
    sizes,
    slides,
    cotangent,
    kernel,
    kernel_bias,
    norm_gain,
    norm_bias,
    weight_in,
    bias_in,
    weight_out,
    bias_out,
    layer_scale,
    out_map,
    out_slides,
    out_in,
    out_out,
    out_small,
    pads,
    gpads,
    taps,
    mixed,
    win,
    wout,
    normed,
    rstd,
    normal,
    normal_t,
    act,
    slope,
    branch,
    upstream,
    gb_low,
    gb_t,
    gnorm,
    gbias,
    mixed_bias,
    grads,
    from_core,
    from_dp,
    from_row,
    from_col,
    early_row,
    early_col,
    early_dp,
    final,
    small,
    small_row,
    small_cd,
    small_out,
    row_send,
    col_send,
    cor_send,
    row_recv,
    col_recv,
    cor_recv,
    cor_wide,
    sem_local,
    sem_ws,
    sem_wr,
    sem_hs,
    sem_hr,
    sem_gs,
    sem_gr,
    sem_ss,
    sem_sr,
    sem_out,
    output,
    grad_slides,
    sem_maps,
):
    R, C, DP = sizes["row"], sizes["col"], sizes["dp"]
    CD = C * DP
    L, NT, _, T, D = wout.shape[0], wout.shape[1], 0, wout.shape[2], wout.shape[3]
    J = D // LANES
    H, W = slides.shape[1], slides.shape[2]
    N = H * W
    DH = D // DP
    UN = DH // UNIT
    row, col, dp = lax.axis_index("row"), lax.axis_index("col"), lax.axis_index("dp")
    cd = col * DP + dp
    core = row % 2

    def remote(src, dst, ssem, rsem, **where):
        return pltpu.make_async_remote_copy(
            src_ref=src,
            dst_ref=dst,
            send_sem=ssem,
            recv_sem=rsem,
            device_id=where,
            device_id_type=MESH,
        )

    def flip(index, bit):
        return index + bit - 2 * bit * ((index // bit) % 2)

    def there(dr, dc):
        ok = True
        if dr:
            ok = (row > 0) if dr < 0 else (row < R - 1)
        if dc:
            side = (col > 0) if dc < 0 else (col < C - 1)
            ok = side if ok is True else jnp.logical_and(ok, side)
        return ok

    def cd_peer(k):
        peer = (cd + k) % CD
        return peer, peer // DP, peer % DP

    barrier = pltpu.get_barrier_semaphore()
    for k in range(1, R):
        pl.semaphore_signal(
            barrier, inc=1, device_id={"row": (row + k) % R}, device_id_type=MESH
        )
    for k in range(1, CD):
        _, pc, pd = cd_peer(k)
        pl.semaphore_signal(
            barrier, inc=1, device_id={"col": pc, "dp": pd}, device_id_type=MESH
        )
    for dr, dc in DIAGONAL:

        @pl.when(there(dr, dc))
        def _():
            pl.semaphore_signal(
                barrier,
                inc=1,
                device_id={"row": row + dr, "col": col + dc},
                device_id_type=MESH,
            )

    own_in = [
        pltpu.make_async_copy(
            weight_in.at[l], win.at[l, pl.ds(dp * DH, DH), :], sem_local.at[l, 0]
        )
        for l in range(L)
    ]
    own_out = [
        pltpu.make_async_copy(
            weight_out.at[l],
            wout.at[l, :, :, pl.ds(dp * DH, DH)],
            sem_local.at[l, 1],
        )
        for l in range(L)
    ]
    for l in range(L):
        own_in[l].start()
        own_out[l].start()

    tall = H + 6
    zero_line = jnp.zeros((W + 2 * LEFT, LANES), F32)

    def clear(i, _):
        for j in range(J):
            for l in range(L):
                pads[l, j, i] = zero_line
                gpads[l, j, i] = zero_line
        return 0

    lax.fori_loop(0, tall, clear, 0)
    small[...] = jnp.zeros_like(small)
    for l in range(L):
        for p in range(7):
            for j in range(J):
                for q in range(7):
                    taps[l, j, 7 * p + q : 7 * p + q + 1, :] = kernel[
                        p, q, l : l + 1, j * LANES : (j + 1) * LANES
                    ]

    def fill(i, _):
        line = slides[0, i].astype(F32)
        for j in range(J):
            pads[0, j, i + 3, LEFT : LEFT + W, :] = line[:, j * LANES : (j + 1) * LANES]
        return 0

    lax.fori_loop(0, H, fill, 0)
    cor_wide[...] = jnp.zeros_like(cor_wide)

    def halo_copy(which, turn):
        if which < 4:
            dr, dc = STRAIGHT[which]
            if dr:
                src, dst = row_send.at[which], row_recv.at[turn, which]
            else:
                src, dst = col_send.at[which - 2], col_recv.at[turn, which - 2]
        else:
            dr, dc = DIAGONAL[which - 4]
            src, dst = cor_send.at[which - 4], cor_recv.at[turn, which - 4]
        where = {}
        if dr:
            where["row"] = row + dr
        if dc:
            where["col"] = col + dc
        return remote(src, dst, sem_hs.at[which], sem_hr.at[turn, which], **where)

    def lanes(j):
        return slice(j * LANES, (j + 1) * LANES)

    def halo_send(turn, src):
        for which, first in ((0, 3), (1, H)):
            for i in range(3):
                for j in range(J):
                    row_send[which, i, :, lanes(j)] = src[
                        j, first + i, LEFT : LEFT + W, :
                    ].astype(BF16)

            @pl.when(there(*STRAIGHT[which]))
            def _():
                halo_copy(which, turn).start()

        for which, first in ((2, LEFT), (3, LEFT + W - 3)):
            for i in range(3):
                for j in range(J):
                    col_send[which - 2, i, :, lanes(j)] = src[
                        j, 3 : 3 + H, first + i, :
                    ].astype(BF16)

            @pl.when(there(*STRAIGHT[which]))
            def _():
                halo_copy(which, turn).start()

        for k, (dr, dc) in enumerate(DIAGONAL):
            first, start = (3 if dr < 0 else H), (LEFT if dc < 0 else LEFT + W - 3)
            for i in range(3):
                for j in range(J):
                    cor_wide[3 * i : 3 * i + 3, lanes(j)] = src[
                        j, first + i, start : start + 3, :
                    ]
            cor_send[k] = cor_wide[...].astype(BF16)

            @pl.when(there(dr, dc))
            def _():
                halo_copy(4 + k, turn).start()

    def halo_recv(turn, dst):
        for which in (0, 1):
            first = H + 3 if which == 0 else 0
            dr, dc = STRAIGHT[which]

            @pl.when(there(-dr, -dc))
            def _():
                halo_copy(which, turn).wait_recv()
                for i in range(3):
                    line = row_recv[turn, which, i].astype(F32)
                    for j in range(J):
                        dst[j, first + i, LEFT : LEFT + W, :] = line[:, lanes(j)]

        for which in (2, 3):
            first = LEFT + W if which == 2 else LEFT - 3
            dr, dc = STRAIGHT[which]

            @pl.when(there(-dr, -dc))
            def _():
                halo_copy(which, turn).wait_recv()
                for i in range(3):
                    line = col_recv[turn, which - 2, i].astype(F32)
                    for j in range(J):
                        dst[j, 3 : 3 + H, first + i, :] = line[:, lanes(j)]

        for k, (dr, dc) in enumerate(DIAGONAL):
            first, start = (H + 3 if dr < 0 else 0), (LEFT + W if dc < 0 else LEFT - 3)

            @pl.when(there(-dr, -dc))
            def _():
                halo_copy(4 + k, turn).wait_recv()
                block = cor_recv[turn, k].astype(F32)
                for i in range(3):
                    for j in range(J):
                        dst[j, first + i, start : start + 3, :] = block[
                            3 * i : 3 * i + 3, lanes(j)
                        ]

        for which in range(8):
            dr, dc = (STRAIGHT + DIAGONAL)[which]

            @pl.when(there(dr, dc))
            def _():
                halo_copy(which, turn).wait_send()

    quarter = row % QUARTERS
    pieces = NT // QUARTERS

    def held(which, l, p, side, q):
        t = q * pieces + p
        if which == 0:
            cols = pl.ds(pl.multiple_of(t * T, T), T)
            return win.at[l, pl.ds(side * DH, DH), cols]
        return wout.at[l, t, :, pl.ds(side * DH, DH)]

    def own(which, l, p):
        t = quarter * pieces + p
        if which == 0:
            return weight_in.at[l, :, pl.ds(pl.multiple_of(t * T, T), T)]
        return weight_out.at[l, t]

    other = 1 - dp

    def w_x(l, which, p):
        k = (l * 2 + which) * pieces + p
        return remote(
            own(which, l, p),
            held(which, l, p, dp, quarter),
            sem_ws.at[0, k],
            sem_wr.at[0, k],
            dp=1 - dp,
        )

    def w_hop(l, which, p, stage):
        k = (l * 2 + which) * pieces + p
        bit = 2 if stage == 1 else 1
        q = flip(quarter, 2) if stage == 3 else quarter
        part = held(which, l, p, other, q)
        return remote(
            part, part, sem_ws.at[stage, k], sem_wr.at[stage, k], row=flip(row, bit)
        )

    def weights_x(l, which):
        for p in range(pieces):
            w_x(l, which, p).start()

    def weights_forward(l, which, p):
        w_x(l, which, p).wait()
        w_hop(l, which, p, 1).start()
        w_hop(l, which, p, 2).start()

    def weights_second(l, which, p):
        w_hop(l, which, p, 1).wait()
        w_hop(l, which, p, 3).start()

    def weights_got(l, which, p, stage):
        w_hop(l, which, p, stage).wait()

    def my_tile(s):
        q, p = s // pieces, s % pieces
        spot = flip(quarter, 1) * (q % 2) + quarter * (1 - q % 2)
        return ((spot + 2 * (q // 2)) % QUARTERS) * pieces + p

    def conv(src, l, mirrored, base, put, during=None):
        blocks = H // 8

        def one(index, _):
            j, start = index // blocks, (index % blocks) * 8
            totals = base(j, start)
            for q in range(7):
                for line in range(14):
                    window = src[
                        j, start + line, LEFT - 3 + q : LEFT - 3 + q + W, :
                    ]
                    for p in range(7):
                        i = line - p
                        if 0 <= i < 8:
                            k = 7 * p + q
                            k = 48 - k if mirrored else k
                            totals[i] = totals[i] + window * taps[l, j, k : k + 1, :]
            put(j, start, totals)
            if during is not None:
                during(index)
            return 0

        lax.fori_loop(0, J * blocks, one, 0)

    def tap_sums(l, first, end, during):
        for q in range(first, end):

            def lane_block(j, _):
                def block(index, totals):
                    start = index * 8
                    totals = list(totals)
                    for part in range(0, W, 8):
                        ups = [
                            gpads[
                                l, j, start + 3 + i, LEFT + part : LEFT + part + 8, :
                            ]
                            for i in range(8)
                        ]
                        for line in range(14):
                            first = LEFT - 3 + part + q
                            window = pads[l, j, start + line, first : first + 8, :]
                            for p in range(7):
                                i = line - p
                                if 0 <= i < 8:
                                    totals[p] = totals[p] + window * ups[i]
                    return tuple(totals)

                zero = jnp.zeros((8, LANES), F32)
                totals = lax.fori_loop(0, H // 8, block, (zero,) * 7)
                for p in range(7):
                    put_small(
                        l, 7 * p + q, j, jnp.sum(totals[p], axis=0, keepdims=True)
                    )
                return 0

            lax.fori_loop(0, J, lane_block, 0)
            during(q)

    M = small.shape[3]

    def put_small(l, line, j, value):
        unit = (line // 8) * J + j
        small[
            l, unit // (CD * M), (unit // M) % CD, unit % M, line % 8 : line % 8 + 1, :
        ] = value

    def put_row(l, line, value):
        for j in range(J):
            put_small(l, line, j, value[:, lanes(j)])

    def transpose(src, dst):
        for k in range(N // LANES):
            block = src[k * LANES : (k + 1) * LANES, :].astype(F32)
            dst[:, lanes(k)] = block.T.astype(BF16)

    def forward(l, last, hooks):
        bias_line = kernel_bias[l : l + 1, :]
        for j in range(J):
            mixed_bias[j] = bias_line[:, lanes(j)]

        def base(j, start):
            del start
            bias = mixed_bias[j]
            return [jnp.broadcast_to(bias, (W, LANES)) for _ in range(8)]

        def put(j, start, totals):
            for i in range(8):
                mixed[j, start + i] = totals[i]

        conv(pads.at[l], l, False, base, put, hooks["conv"])
        hooks["conv"](-1)
        gain, shift = norm_gain[l : l + 1, :], norm_bias[l : l + 1, :]

        def norm(i, _):
            lines = pl.ds(i * W, W)
            value = jnp.concatenate([mixed[j, i] for j in range(J)], axis=1)
            center = value - jnp.mean(value, -1, keepdims=True)
            scale = lax.rsqrt(jnp.mean(center * center, -1, keepdims=True) + EPSILON)
            out = center * scale
            normed[l, lines, :] = out
            rstd[l, lines, :] = scale
            normal[lines, :] = (out * gain + shift).astype(BF16)
            return 0

        lax.fori_loop(0, H, norm, 0, unroll=4)
        hooks["norm"]()
        transpose(normal, normal_t.at[l])

        group = hooks["group"]

        def expand(s, _):
            hooks["expand"](s)
            for k in range(group):
                t = my_tile(s * group + k)
                cols = pl.ds(pl.multiple_of(t * T, T), T)
                hidden = jnp.dot(normal[...], win[l, :, cols], preferred_element_type=F32)
                hidden = hidden + bias_in[l : l + 1, cols]
                square = hidden * hidden
                tangent = jnp.tanh(hidden * (COEF + (COEF * CUBIC) * square))
                both = 1.0 + tangent
                half = 0.5 * hidden
                act[l, t] = (half * both).astype(BF16)
                steep = half * (COEF + (3.0 * COEF * CUBIC) * square)
                slope[l, t] = (both * (0.5 + (1.0 - tangent) * steep)).astype(BF16)
            return 0

        lax.fori_loop(0, NT // group, expand, 0)
        branch[l] = jnp.broadcast_to(bias_out[l : l + 1, :], (N, D))

        def project(s, _):
            hooks["project"](s)
            total = branch[l]
            for p in range(pieces):
                t = my_tile(s * pieces + p)
                total = total + jnp.dot(
                    act[l, t], wout[l, t], preferred_element_type=F32
                )
            branch[l] = total
            return 0

        lax.fori_loop(0, QUARTERS, project, 0)
        scales = layer_scale[l : l + 1, :]

        def finish(i, _):
            part = scales * branch[l, pl.ds(i * W, W), :]
            for j in range(J):
                old = pads[l, j, i + 3, LEFT : LEFT + W, :]
                new = (old + part[:, lanes(j)]).astype(BF16)
                if last:
                    output[0, i, :, lanes(j)] = new
                else:
                    pads[l + 1, j, i + 3, LEFT : LEFT + W, :] = new.astype(F32)
            return 0

        lax.fori_loop(0, H, finish, 0)
        if last:
            map_copy.start()

    bits = []
    bit = 2
    while bit < R:
        bits.append(bit)
        bit *= 2
    levels = []
    count = UN
    for b in bits:
        halve = count // 2 >= C
        levels.append((b, count, halve))
        count = count // 2 if halve else count
    left_units = count
    per_col = left_units // C
    nb = len(bits)
    S_CORE, S_DP, S_ROW, S_COL = 0, 1, 2, 2 + nb
    S_COLG = S_COL + C - 1
    S_ROWG = S_COLG + C - 1
    S_COREG = S_ROWG + nb

    def unit_base(level):
        start = 0
        for b, n, halve in levels[:level]:
            if halve:
                start = start + ((row // b) % 2) * (n // 2)
        return start

    def g_core(l, t):
        return remote(
            grads.at[l, t, 1 - core],
            from_core.at[l, t],
            sem_gs.at[t, S_CORE],
            sem_gr.at[l, t, S_CORE],
            row=flip(row, 1),
        )

    def g_dp(l, t):
        return remote(
            grads.at[l, t, core, 1 - dp],
            from_dp.at[l, t],
            sem_gs.at[t, S_DP],
            sem_gr.at[l, t, S_DP],
            dp=1 - dp,
        )

    row_slot = []
    at = 0
    for b, n, halve in levels:
        row_slot.append(at)
        at += n // 2 if halve else n

    def g_row(l, t, level):
        b, n, halve = levels[level]
        mine = (row // b) % 2
        start = unit_base(level)
        m = n
        if halve:
            m = n // 2
            start = start + (1 - mine) * m
        return remote(
            grads.at[l, t, core, dp, pl.ds(start, m)],
            from_row.at[l, t, pl.ds(row_slot[level], m)],
            sem_gs.at[t, S_ROW + level],
            sem_gr.at[l, t, S_ROW + level],
            row=flip(row, b),
        )

    def g_row_add(l, t, level):
        b, n, halve = levels[level]
        start = unit_base(level + 1)
        m = n // 2 if halve else n
        mine = grads.at[l, t, core, dp, pl.ds(start, m)]
        mine[...] = mine[...] + from_row[l, t, pl.ds(row_slot[level], m)]

    col_base = unit_base(nb)

    def g_col(l, t, k):
        peer = (col + k) % C
        return remote(
            grads.at[l, t, core, dp, pl.ds(col_base + peer * per_col, per_col)],
            from_col.at[l, t, k - 1],
            sem_gs.at[t, S_COL + k - 1],
            sem_gr.at[l, t, S_COL + k - 1],
            col=peer,
        )

    def g_colg(l, t, k):
        peer = (col + k) % C
        part = final.at[l, core, t, pl.ds(col_base + col * per_col, per_col)]
        return remote(
            part,
            part,
            sem_gs.at[t, S_COLG + k - 1],
            sem_gr.at[l, t, S_COLG + k - 1],
            col=peer,
        )

    def g_rowg(l, t, level):
        b, n, halve = levels[level]
        part = final.at[l, core, t, pl.ds(unit_base(level + 1), n // 2)]
        return remote(
            part,
            part,
            sem_gs.at[t, S_ROWG + level],
            sem_gr.at[l, t, S_ROWG + level],
            row=flip(row, b),
        )

    def g_coreg(l, t):
        part = final.at[l, core, t]
        return remote(
            part,
            part,
            sem_gs.at[t, S_COREG],
            sem_gr.at[l, t, S_COREG],
            row=flip(row, 1),
        )

    def go_dp(l, t):
        g_core(l, t).wait()
        mine = grads.at[l, t, core]
        mine[...] = mine[...] + from_core[l, t]
        g_dp(l, t).start()

    def go_row(l, t):
        g_dp(l, t).wait()
        mine = grads.at[l, t, core, dp]
        mine[...] = mine[...] + from_dp[l, t]
        for level in range(nb):
            if level:
                g_row(l, t, level - 1).wait()
                g_row_add(l, t, level - 1)
            g_row(l, t, level).start()

    def go_col(l, t):
        if nb:
            g_row(l, t, nb - 1).wait()
            g_row_add(l, t, nb - 1)
        for k in range(1, C):
            g_col(l, t, k).start()

    def go_colg(l, t):
        for k in range(1, C):
            g_col(l, t, k).wait()
        place = pl.ds(col_base + col * per_col, per_col)
        total = grads[l, t, core, dp, place].astype(F32)
        for k in range(1, C):
            total = total + from_col[l, t, k - 1].astype(F32)
        final[l, core, t, place] = total.astype(BF16)
        for k in range(1, C):
            g_colg(l, t, k).start()

    halved = [k for k in range(nb) if levels[k][2]][::-1]

    def go_rowg(l, t):
        for k in range(1, C):
            g_colg(l, t, k).wait()
        for n, level in enumerate(halved):
            if n:
                g_rowg(l, t, halved[n - 1]).wait()
            g_rowg(l, t, level).start()

    def go_coreg(l, t):
        if halved:
            g_rowg(l, t, halved[-1]).wait()
        g_coreg(l, t).start()

    def h_row(l, t, level):
        b, n, halve = levels[level]
        start, m = unit_base(level), n
        if halve:
            m = n // 2
            start = start + (1 - (row // b) % 2) * m
        return remote(
            grads.at[l, t, core, :, pl.ds(start, m)],
            early_row.at[t, :, pl.ds(row_slot[level], m)],
            sem_gs.at[t, S_ROW + level],
            sem_gr.at[l, t, S_ROW + level],
            row=flip(row, b),
        )

    def h_row_add(l, t, level):
        _, n, halve = levels[level]
        m = n // 2 if halve else n
        mine = grads.at[l, t, core, :, pl.ds(unit_base(level + 1), m)]
        mine[...] = mine[...] + early_row[t, :, pl.ds(row_slot[level], m)]

    def h_col(l, t, k):
        peer = (col + k) % C
        return remote(
            grads.at[l, t, core, :, pl.ds(col_base + peer * per_col, per_col)],
            early_col.at[t, k - 1],
            sem_gs.at[t, S_COL + k - 1],
            sem_gr.at[l, t, S_COL + k - 1],
            col=peer,
        )

    my_units = pl.ds(col_base + col * per_col, per_col)

    def h_dp(l, t):
        return remote(
            grads.at[l, t, core, 1 - dp, my_units],
            early_dp.at[t],
            sem_gs.at[t, S_DP],
            sem_gr.at[l, t, S_DP],
            dp=1 - dp,
        )

    def early_start(l, t):
        g_core(l, t).wait()
        mine = grads.at[l, t, core]
        mine[...] = mine[...] + from_core[l, t]
        for level in range(nb):
            if level:
                h_row(l, t, level - 1).wait()
                h_row_add(l, t, level - 1)
            h_row(l, t, level).start()

    def early_col_go(l, t):
        if nb:
            h_row(l, t, nb - 1).wait()
            h_row_add(l, t, nb - 1)
        for k in range(1, C):
            h_col(l, t, k).start()

    def early_dp_go(l, t):
        for k in range(1, C):
            h_col(l, t, k).wait()
        total = grads[l, t, core, :, my_units].astype(F32)
        for k in range(1, C):
            total = total + early_col[t, k - 1].astype(F32)
        grads[l, t, core, :, my_units] = total.astype(BF16)
        h_dp(l, t).start()

    def early_colg(l, t):
        h_dp(l, t).wait()
        final[l, core, t, my_units] = grads[l, t, core, dp, my_units] + early_dp[t]
        for k in range(1, C):
            g_colg(l, t, k).start()

    def out_copies(l, t):
        cols = pl.ds(pl.multiple_of(t * T, T), T)
        return (
            pltpu.make_async_copy(
                final.at[l, 0, t], out_in.at[l, :, :, cols], sem_out.at[0, l, t]
            ),
            pltpu.make_async_copy(
                final.at[l, 1, t], out_out.at[l, :, :, cols], sem_out.at[1, l, t]
            ),
        )

    def go_out(l, t):
        g_coreg(l, t).wait()
        for copy in out_copies(l, t):
            copy.start()

    chain = (go_row, go_col, go_colg, go_rowg, go_coreg, go_out)

    def s_copy(l, stage, k):
        if stage in (0, 3):
            peer = (row + k) % R
            where = {"row": peer}
        else:
            peer, pc, pd = cd_peer(k)
            where = {"col": pc, "dp": pd}
        if stage == 0:
            src, dst = small.at[l, peer], small_row.at[l, k - 1]
        elif stage == 1:
            src, dst = small.at[l, row, peer], small_cd.at[l, k - 1]
        elif stage == 2:
            src = dst = small_out.at[l, row, cd]
        else:
            src = dst = small_out.at[l, row]
        return remote(
            src, dst, sem_ss.at[stage, k - 1], sem_sr.at[l, stage, k - 1], **where
        )

    def small_copy(l):
        return pltpu.make_async_copy(
            small_out.at[l], out_small.at[l], sem_maps.at[2 + l]
        )

    map_copy = pltpu.make_async_copy(output, out_map, sem_maps.at[0])
    slides_copy = pltpu.make_async_copy(grad_slides, out_slides, sem_maps.at[1])

    def small_start(l):
        for k in range(1, R):
            s_copy(l, 0, k).start()

    def small_second(l):
        for k in range(1, R):
            s_copy(l, 0, k).wait()
        total = small[l, row]
        for k in range(1, R):
            total = total + small_row[l, k - 1]
        small[l, row] = total
        for k in range(1, CD):
            s_copy(l, 1, k).start()

    def small_third(l):
        for k in range(1, CD):
            s_copy(l, 1, k).wait()
        total = small[l, row, cd]
        for k in range(1, CD):
            total = total + small_cd[l, k - 1]
        small_out[l, row, cd] = total
        for k in range(1, CD):
            s_copy(l, 2, k).start()

    def small_fourth(l):
        for k in range(1, CD):
            s_copy(l, 2, k).wait()
        for k in range(1, R):
            s_copy(l, 3, k).start()

    def small_end(l):
        for k in range(1, R):
            s_copy(l, 3, k).wait()
        small_copy(l).start()

    def backward(l, turn, hooks, last):
        gpad = gpads.at[l]
        scales = layer_scale[l : l + 1, :]
        empty = jnp.zeros((8, D), F32)

        def fold(value):
            total = value[0:8]
            for k in range(8, value.shape[0], 8):
                total = total + value[k : k + 8]
            return total

        def before(i, sums):
            lines = pl.ds(i * W, W)
            up = upstream[lines, :]
            gb = up * scales
            gb_low[lines, :] = gb.astype(BF16)
            return (sums[0] + fold(up * branch[l, lines, :]), sums[1] + fold(gb))

        sums = lax.fori_loop(0, H, before, (empty,) * 2)
        put_row(l, 53, jnp.sum(sums[0], 0, keepdims=True))
        put_row(l, 52, jnp.sum(sums[1], 0, keepdims=True))
        gnorm[...] = jnp.zeros_like(gnorm)
        transpose(gb_low, gb_t)

        def pair(i, _):
            first_late = 2
            if l == L - 1:
                first_late = 3

                @pl.when(i == 2)
                def _():
                    for k in range(PAIR):
                        early_start(l, k)

            @pl.when(i >= first_late)
            def _():
                for k in range(PAIR):
                    go_dp(l, (i - 2) * PAIR + k)

            hooks('tile', i)
            gb, gb_turned = gb_low[...], gb_t[...]
            lows = []
            for k in range(PAIR):
                t = i * PAIR + k
                ga = lax.dot_general(gb, wout[l, t], COLS, preferred_element_type=F32)
                gh = ga * slope[l, t].astype(F32)
                gbias[t] = jnp.sum(gh, 0, keepdims=True)
                lows.append(gh.astype(BF16))
            for k in range(PAIR):
                t = i * PAIR + k
                g_out = jnp.dot(gb_turned, act[l, t], preferred_element_type=F32)
                grads[l, t, 1] = g_out.astype(BF16).reshape(DP, UN, UNIT, T)
            total = gnorm[...]
            for k in range(PAIR):
                t = i * PAIR + k
                g_in = jnp.dot(normal_t[l], lows[k], preferred_element_type=F32)
                grads[l, t, 0] = g_in.astype(BF16).reshape(DP, UN, UNIT, T)
                cols = pl.ds(pl.multiple_of(t * T, T), T)
                total = total + lax.dot_general(
                    lows[k], win[l, :, cols], COLS, preferred_element_type=F32
                )
            gnorm[...] = total
            for k in range(PAIR):
                g_core(l, i * PAIR + k).start()
            return 0

        lax.fori_loop(0, NT // PAIR, pair, 0)
        for t in range(NT - 2 * PAIR, NT - PAIR):
            go_dp(l, t)
        hooks('rest', -1)
        per_line = D // T
        for t in range(NT):
            for half in range(T // LANES):
                j = (t % per_line) * (T // LANES) + half
                put_small(l, 54 + t // per_line, j, gbias[t, :, lanes(half)])
        gain = norm_gain[l : l + 1, :]

        def after(i, sums):
            lines = pl.ds(i * W, W)
            gn, unit = gnorm[lines, :], normed[l, lines, :]
            both = gn * unit
            gs = gn * gain
            first = jnp.mean(gs, -1, keepdims=True)
            second = jnp.mean(gs * unit, -1, keepdims=True)
            gm = rstd[l, lines, :] * (gs - first - unit * second)
            for j in range(J):
                gpad[j, i + 3, LEFT : LEFT + W, :] = gm[:, lanes(j)]
            return (sums[0] + fold(gm), sums[1] + fold(both), sums[2] + fold(gn))

        sums = lax.fori_loop(0, H, after, (empty,) * 3, unroll=2)
        for k in range(3):
            put_row(l, 49 + k, jnp.sum(sums[k], 0, keepdims=True))
        halo_send(turn, gpad)
        for t in range(NT - PAIR, NT):
            go_dp(l, t)
        hooks('sent', -1)
        halo_recv(turn, gpad)

        def base(j, start):
            return [up_block[j, start + i] for i in range(8)]

        up_block = mixed

        def spread(i, _):
            for j in range(J):
                mixed[j, i] = upstream[pl.ds(i * W, W), lanes(j)]
            return 0

        lax.fori_loop(0, H, spread, 0)

        def put(j, start, totals):
            for i in range(8):
                mixed[j, start + i] = totals[i]

        conv(gpad, l, True, base, put, lambda k: hooks('conv', k))

        def gather(i, _):
            for j in range(J):
                if last:
                    grad_slides[0, i, :, lanes(j)] = mixed[j, i].astype(BF16)
                else:
                    upstream[pl.ds(i * W, W), lanes(j)] = mixed[j, i]
            return 0

        lax.fori_loop(0, H, gather, 0)
        if last:
            slides_copy.start()

    diagonals = jnp.where(row > 0, 1, 0) + jnp.where(row < R - 1, 1, 0)
    diagonals = diagonals * (
        jnp.where(col > 0, 1, 0) + jnp.where(col < C - 1, 1, 0)
    )
    pl.semaphore_wait(barrier, R - 1 + CD - 1 + diagonals)
    halo_send(0, pads.at[0])
    for l in range(L):
        for which in range(2):
            weights_x(l, which)
    halo_recv(0, pads.at[0])

    def start_up(i, _):
        upstream[pl.ds(i * W, W), :] = cotangent[0, i].astype(F32)
        return 0

    lax.fori_loop(0, H, start_up, 0)

    def at(value, index, call):
        @pl.when(value == index)
        def _():
            call()

    blocks = J * (H // 8)
    spread_out = [(k, max(blocks * (2 * k + 1) // (2 * pieces), 1)) for k in range(pieces)]

    def first_conv(index):
        if not isinstance(index, int):
            for p, place in spread_out:
                at(index, place, lambda: weights_forward(0, 0, p))

    def first_norm():
        weights_got(0, 0, 0, 2)
        own_in[0].wait()

    def first_expand(s):
        def second(p):
            weights_second(0, 0, p)

        for p in range(pieces):
            if p:
                at(s, pieces + p, lambda: weights_got(0, 0, p, 2))
            at(s, 2 * pieces - 1 + p, lambda: second(p))
            at(s, 3 * pieces + p, lambda: weights_got(0, 0, p, 3))
            at(s, (2 * p + 1) * pieces, lambda: weights_forward(0, 1, p))

    def first_project(s):
        def one():
            for p in range(pieces):
                weights_got(0, 1, p, 2)

        def two():
            for p in range(pieces):
                weights_second(0, 1, p)

        def three():
            for p in range(pieces):
                weights_got(0, 1, p, 3)

        at(s, 0, lambda: own_out[0].wait())
        at(s, 1, one)
        at(s, 2, two)
        at(s, 3, three)
        if L > 1:
            for p in range(pieces):
                at(s, min(1 + p, QUARTERS - 1), lambda: weights_forward(1, 0, p))

    def later(l):
        def in_conv(index):
            if isinstance(index, int):
                weights_second(l, 0, pieces - 1)
                return
            for p in range(pieces):
                at(index, min(1 + 3 * p, blocks - 1), lambda: weights_forward(l, 1, p))
                if p + 1 < pieces:
                    at(index, blocks - 2, lambda: weights_second(l, 0, p))

        def in_norm():
            for p in range(pieces):
                weights_got(l, 0, p, 2)
                weights_got(l, 0, p, 3)
            own_in[l].wait()

        def in_expand(s):
            for p in range(pieces):
                at(s, min(1 + 2 * p, QUARTERS - 1), lambda: weights_second(l, 1, p))

        def in_project(s):
            def one():
                for p in range(pieces):
                    weights_got(l, 1, p, 2)
                own_out[l].wait()

            def three():
                for p in range(pieces):
                    weights_got(l, 1, p, 3)

            at(s, 0, one)
            at(s, 3, three)

        return dict(
            conv=in_conv,
            norm=in_norm,
            expand=in_expand,
            project=in_project,
            group=pieces,
        )

    first = dict(
        conv=first_conv,
        norm=first_norm,
        expand=first_expand,
        project=first_project,
        group=1,
    )
    for l in range(L):
        if l:
            for p in range(pieces if l > 1 else 0):
                weights_forward(l, 0, p)
            halo_recv(l, pads.at[l])
        forward(l, l == L - 1, later(l) if l else first)
        if l + 1 < L:
            halo_send(l + 1, pads.at[l + 1])

    clock = [0.0]
    due = []
    link = [0.0]
    serial = [0]
    cross = [0.0]

    def push(ready, chain, place, arg):
        serial[0] += 1
        due.append((ready, serial[0], chain, place, arg))

    gchain = [
        (go_row, 4.0),
        (go_col, 4.8),
        (go_colg, 4.8),
        (go_rowg, 4.0),
        (go_coreg, 9.0),
        (go_out, 0.0),
    ]
    echain = [(early_col_go, 4.8), (early_dp_go, 5.4), (early_colg, 3.5)] + gchain[3:]
    echain[2] = (early_colg, 3.5)
    schain = [(small_second, 6.0), (small_third, 7.0), (small_fourth, 7.0), (small_end, 0)]

    def run_due(now):
        while due:
            best = min(due)
            if best[0] > now:
                return
            due.remove(best)
            ready, _, chain, place, arg = best
            chain[place][0](*arg)
            if place + 1 < len(chain):
                wait = chain[place][1]
                soon = max(ready, clock[0]) + wait
                if chain is echain and place == 1:
                    link[0] = max(link[0], clock[0]) + 0.35
                    soon = link[0] + 3.0
                if chain is schain and place == 0:
                    soon = max(soon, link[0] + 4.0)
                push(soon, chain, place + 1, arg)

    def spend(time):
        clock[0] += time
        run_due(clock[0])

    TILE, CONV, TAP = 1.4, 0.57, 0.75
    cut = 6
    for n, l in enumerate(reversed(range(L))):
        last = l == 0

        def hooks(name, index, l=l, last=last):
            if name == 'tile':
                start = clock[0]
                for t in range(NT // PAIR):
                    clock[0] = start + t * TILE
                    ready_now = [x for x in due if x[0] <= clock[0]]
                    if ready_now:
                        at(index, t, lambda: run_due(clock[0]))
                clock[0] = start + TILE * NT // PAIR
                for t in range(NT):
                    begin = start + TILE * min(t // PAIR + 2, NT // PAIR)
                    if l == L - 1 and t < PAIR:
                        cross[0] = max(cross[0], begin) + 2.75
                        push(cross[0] + 2.3, echain, 0, (l, t))
                        continue
                    begin = max(link[0], begin)
                    link[0] = begin + 2.75
                    push(link[0] + 2.3, gchain, 0, (l, t))
            elif name == 'rest':
                spend(0.8)
            elif name == 'sent':
                spend(1.4)
                if last:
                    for k in range(1, L):
                        tap_sums(k, cut, 7, lambda q: spend(TAP))
                        small_start(k)
                        push(clock[0] + 7.0, schain, 0, (k,))
                    tap_sums(l, 0, 7, lambda q: spend(TAP))
                    small_start(l)
                    push(clock[0] + 8.0, schain, 0, (l,))
                else:
                    tap_sums(l, 0, cut, lambda q: spend(TAP))
            elif name == 'conv':
                start = clock[0]
                for k in range(blocks):
                    clock[0] = start + (k + 1) * CONV
                    if [x for x in due if x[0] <= clock[0]]:
                        at(index, k, lambda: run_due(clock[0]))

        backward(l, L + n, hooks, last)
        spend(0.8)
    while due:
        clock[0] = max(clock[0], min(due)[0])
        run_due(clock[0])
    def drain(t, _):
        for l in range(L):
            for copy in out_copies(l, t):
                copy.wait()
        return 0

    lax.fori_loop(0, NT, drain, 0)
    map_copy.wait()
    slides_copy.wait()
    for l in range(L):
        small_copy(l).wait()


def per_device(
    sizes,
    slides,
    cotangent,
    kernel,
    kernel_bias,
    norm_gain,
    norm_bias,
    weight_in,
    bias_in,
    weight_out,
    bias_out,
    layer_scale,
):
    R, C, DP = sizes["row"], sizes["col"], sizes["dp"]
    CD = C * DP
    L, DH, FF = weight_in.shape
    D = slides.shape[-1]
    H, W = slides.shape[1], slides.shape[2]
    N = H * W
    J = D // LANES
    T = DH
    NT = FF // T
    UN = DH // UNIT
    everyone = R * CD
    need = -(-(54 + FF // D) // 8) * J
    M = -(-need // everyone)
    row_units, count, bit, nb = 0, UN, 2, 0
    while bit < R:
        halve = count // 2 >= C
        count = count // 2 if halve else count
        row_units += count
        bit *= 2
        nb += 1
    per_col = count // C
    early = PAIR
    stages = 2 + nb + 2 * (C - 1) + nb + 1
    small_peers = max(R, CD) - 1
    vmem = pl.BlockSpec(memory_space=pltpu.VMEM)
    hbm = pl.BlockSpec(memory_space=pl.ANY)
    V = pltpu.VMEM
    DMA = pltpu.SemaphoreType.DMA
    turns = 2 * L
    out = pl.pallas_call(
        functools.partial(step_body, sizes),
        out_shape=(
            jax.ShapeDtypeStruct((1, H, W, D), BF16),
            jax.ShapeDtypeStruct((1, H, W, D), BF16),
            jax.ShapeDtypeStruct((L, UN, UNIT, FF), BF16),
            jax.ShapeDtypeStruct((L, UN, UNIT, FF), BF16),
            jax.ShapeDtypeStruct((L, R, CD, M, 8, LANES), F32),
        ),
        in_specs=[vmem] * 6 + [hbm, vmem, hbm, vmem, vmem],
        out_specs=(hbm,) * 5,
        scratch_shapes=[
            V((L, J, H + 6, W + 2 * LEFT, LANES), F32),
            V((L, J, H + 6, W + 2 * LEFT, LANES), F32),
            V((L, J, 49, LANES), F32),
            V((J, H, W, LANES), F32),
            V((L, D, FF), BF16),
            V((L, NT, T, D), BF16),
            V((L, N, D), F32),
            V((L, N, 1), F32),
            V((N, D), BF16),
            V((L, D, N), BF16),
            V((L, NT, N, T), BF16),
            V((L, NT, N, T), BF16),
            V((L, N, D), F32),
            V((N, D), F32),
            V((N, D), BF16),
            V((D, N), BF16),
            V((N, D), F32),
            V((NT, 1, T), F32),
            V((J, 1, LANES), F32),
            V((L, NT, 2, DP, UN, UNIT, T), BF16),
            V((L, NT, DP, UN, UNIT, T), BF16),
            V((L, NT, UN, UNIT, T), BF16),
            V((L, NT, max(row_units, 1), UNIT, T), BF16),
            V((L, NT, max(C - 1, 1), per_col, UNIT, T), BF16),
            V((early, DP, max(row_units, 1), UNIT, T), BF16),
            V((early, max(C - 1, 1), DP, per_col, UNIT, T), BF16),
            V((early, per_col, UNIT, T), BF16),
            V((L, 2, NT, UN, UNIT, T), BF16),
            V((L, R, CD, M, 8, LANES), F32),
            V((L, max(R - 1, 1), CD, M, 8, LANES), F32),
            V((L, max(CD - 1, 1), M, 8, LANES), F32),
            V((L, R, CD, M, 8, LANES), F32),
            V((2, 3, W, D), BF16),
            V((2, 3, H, D), BF16),
            V((4, UNIT, D), BF16),
            V((turns, 2, 3, W, D), BF16),
            V((turns, 2, 3, H, D), BF16),
            V((turns, 4, UNIT, D), BF16),
            V((UNIT, D), F32),
            DMA((L, 2)),
            DMA((4, 4 * L)),
            DMA((4, 4 * L)),
            DMA((8,)),
            DMA((turns, 8)),
            DMA((NT, stages)),
            DMA((L, NT, stages)),
            DMA((4, small_peers)),
            DMA((L, 4, small_peers)),
            DMA((2, L, NT)),
            V((1, H, W, D), BF16),
            V((1, H, W, D), BF16),
            DMA((2 + L,)),
        ],
        compiler_params=pltpu.CompilerParams(
            collective_id=0, has_side_effects=True, vmem_limit_bytes=67043328
        ),
        name="step",
    )(
        slides,
        cotangent,
        kernel.transpose(1, 2, 0, 3),
        kernel_bias,
        norm_gain,
        norm_bias,
        weight_in,
        bias_in,
        weight_out.reshape(L, NT, T, DH),
        bias_out,
        layer_scale,
    )
    return widen(*out, FF)


def widen_body(output, grad_slides, low_in, low_out, small, *outs):
    outs[0][...] = output[...]
    outs[1][...] = grad_slides[...]
    outs[2][...] = low_in[...].astype(F32)
    outs[3][0] = low_out[0].astype(F32).T
    taps, channel, bias = outs[4:]

    @pl.when(pl.program_id(0) == 0)
    def _():
        L, D = channel.shape[1], channel.shape[2]
        J = D // LANES
        for l in range(L):
            for line in range(54 + bias.shape[1] // D):
                for j in range(J):
                    unit = (line // 8) * J + j
                    value = small[l, unit, line % 8 : line % 8 + 1, :]
                    lane = j * LANES
                    if line < 49:
                        taps[
                            line // 7, line % 7, l : l + 1, lane : lane + LANES
                        ] = value
                    elif line < 54:
                        channel[line - 49, l : l + 1, lane : lane + LANES] = value
                    else:
                        lane += (line - 54) * D
                        bias[l : l + 1, lane : lane + LANES] = value


def widen(output, grad_slides, low_in, low_out, small, FF):
    _, H, W, D = output.shape
    L, DH = low_in.shape[0], low_in.shape[1] * low_in.shape[2]
    small = small.reshape(L, -1, 8, LANES)
    low_in = low_in.reshape(L, DH, FF)
    low_out = low_out.reshape(L, DH, FF)
    parts = 2
    steps = L * parts
    rows = -(-H // steps)
    maps = pl.BlockSpec((1, rows, W, D), lambda i: (0, i, 0, 0))
    wide = pl.BlockSpec((1, DH // parts, FF), lambda i: (i // parts, i % parts, 0))
    long = pl.BlockSpec((1, FF // parts, DH), lambda i: (i // parts, i % parts, 0))
    flat = pl.BlockSpec((1, DH, FF // parts), lambda i: (i // parts, 0, i % parts))

    def whole(shape):
        return pl.BlockSpec(shape, lambda i: (0,) * len(shape))

    shapes = (
        jax.ShapeDtypeStruct(output.shape, BF16),
        jax.ShapeDtypeStruct(output.shape, BF16),
        jax.ShapeDtypeStruct(low_in.shape, F32),
        jax.ShapeDtypeStruct((L, FF, DH), F32),
        jax.ShapeDtypeStruct((7, 7, L, D), F32),
        jax.ShapeDtypeStruct((5, L, D), F32),
        jax.ShapeDtypeStruct((L, FF), F32),
    )
    outs = pl.pallas_call(
        widen_body,
        grid=(steps,),
        out_shape=shapes,
        in_specs=[maps, maps, wide, flat, whole(small.shape)],
        out_specs=(maps, maps, wide, long) + tuple(whole(x.shape) for x in shapes[4:]),
        name="widen",
    )(output, grad_slides, low_in, low_out, small)
    return (
        *outs[:4],
        outs[4].transpose(2, 0, 1, 3),
        outs[5].transpose(1, 0, 2),
        outs[6],
    )


def solution(mesh):
    return jax.shard_map(
        functools.partial(per_device, dict(mesh.shape)),
        mesh=mesh,
        in_specs=(
            P("dp", "row", "col", None),
            P("dp", "row", "col", None),
            P(),
            P(),
            P(),
            P(),
            P(None, "dp", None),
            P(),
            P(None, None, "dp"),
            P(),
            P(),
        ),
        out_specs=(
            P("dp", "row", "col", None),
            P("dp", "row", "col", None),
            P(None, "dp", None),
            P(None, None, "dp"),
            P(),
            P(),
            P(),
        ),
        check_vma=False,
    )
```
